256 devices in a mesh: dp: 16 (over z_hi, x), tp: 16 (over z_lo, y, core).
Axes of the slice: x: 4, y: 4, z: 8 (z_hi: 4, z_lo: 2; z = z_hi * 2 + z_lo), core: 2. Of those that a mesh axis runs over, the one named last changes fastest.
Arguments:
- gradients: bfloat16 [16, 4, 5120, 1280], P('dp', None, 'tp'), may hold values from -6 to 6
- right_factor: float32 [4, 1280, 32], replicated, may hold values from -6 to 6
- weights_before: float32 [4, 5120, 1280], P(None, 'tp', 'dp'), may hold values from -0.15625 to 0.15625
- momentum: float32 [4, 5120, 1280], P(None, 'tp', 'dp'), may hold values from -0.3125 to 0.3125
Outputs:
- new_weights: float32 [4, 5120, 1280], P(None, 'tp', 'dp')
- new_basis: float32 [4, 1280, 32], replicated
- new_momentum: float32 [4, 5120, 1280], P(None, 'tp', 'dp')
The draws below stay inside these ranges and needn't reach their ends.
All inputs are finite; a program needn't handle non-finite values.
Results may differ from the reference program's by a relative error of at most 0.003.
Values sent between devices are 32-bit elements; how exact they have to be, the bound alone decides.
No kernel may reach another device: no remote copies, remote signals or barrier semaphores. Data moves between devices by JAX's collectives and lax.ppermute only.
A program may use at most 64 MiB of HBM per device.

```python
import jax
import jax.numpy as jnp
from jax import lax

WIDTH = 1280
INNER = 5120
RANK = 32
LAYERS = 4
REPLICAS = 16
N_TP = 16


def draw_gradients(key, part):
    keys = jax.random.split(key, 5)
    level = jnp.exp(jax.random.uniform(keys[4], (1, LAYERS, N_TP, 1, RANK), jnp.float32, -1.3, 1.3))
    left = jax.random.normal(keys[0], (1, LAYERS, N_TP, INNER // N_TP, RANK), jnp.float32) * level
    left = left.reshape(1, LAYERS, INNER, RANK)
    right = jax.random.normal(keys[1], (1, LAYERS, RANK, WIDTH), jnp.float32)
    strength = jax.random.normal(keys[2], (REPLICAS, LAYERS, 1, RANK), jnp.float32)
    noise = jax.random.normal(keys[3], (REPLICAS, LAYERS, INNER, WIDTH), jnp.float32)
    low = jnp.einsum('alir,lrw->aliw', left * strength, right[0])
    values = low * RANK ** (-0.5) + 0.5 * noise
    return jnp.clip(values, -6.0, 6.0).astype(jnp.bfloat16)


def block_levels(key, extent, cuts, least, largest):
    def one(position, blocks):
        steps = jax.random.uniform(jax.random.fold_in(jax.random.fold_in(key, 6), position), (blocks,), jnp.float32, least / len(cuts), largest / len(cuts))
        return jnp.repeat(jnp.exp(steps), extent[position] // blocks).reshape((-1,) + (1,) * (len(extent) - position - 1))

    gain = one(*cuts[0])
    for cut in cuts[1:]:
        gain = gain * one(*cut)
    return gain


def gaussian(stream_key, shape, scale, bound, cuts=(), held_as=jnp.bfloat16):
    values = jax.random.normal(stream_key, shape, jnp.float32) * scale
    if len(cuts) > 0:
        values = block_levels(stream_key, shape, cuts, -0.22, 0.18) * values
    return jnp.clip(values, min=-bound, max=bound).astype(held_as)


def setup_inputs(seed: int = 0) -> dict:
    arg_keys = jax.random.split(jax.random.key(seed), 5)
    gradients = draw_gradients(jax.random.fold_in(arg_keys[4], 71), 0)
    right_factor = gaussian(arg_keys[1], (LAYERS, WIDTH, RANK), 1.0, 6.0, (), jnp.float32)
    weights_before = gaussian(arg_keys[2], (LAYERS, INNER, WIDTH), WIDTH ** -0.5, 0.15625, ((1, 16), (2, 16)), jnp.float32)
    momentum = gaussian(arg_keys[3], (LAYERS, INNER, WIDTH), 0.05, 0.3125, ((1, 16), (2, 16)), jnp.float32)
    return {"gradients": gradients, "right_factor": right_factor, "weights_before": weights_before, "momentum": momentum}


def reference(gradients, right_factor, weights_before, momentum):
    small_basis = right_factor.astype(jnp.bfloat16)
    small_basis = lax.optimization_barrier(small_basis)
    left = jnp.einsum('aliw,lwr->lir', gradients.astype(jnp.float32), small_basis.astype(jnp.float32))
    gram = jnp.einsum('lir,lis->lrs', left, left, precision=lax.Precision.HIGHEST)
    gram = gram + 0.001 * lax.optimization_barrier(jnp.mean(jnp.diagonal(gram, axis1=1, axis2=2), axis=1))[:, None, None] * jnp.eye(RANK, dtype=jnp.float32)
    small_left = lax.optimization_barrier(left.astype(jnp.bfloat16))
    right = jnp.einsum('aliw,lir->lwr', gradients.astype(jnp.float32), small_left.astype(jnp.float32))
    root = jnp.linalg.cholesky(gram)
    half = lax.linalg.triangular_solve(root, jnp.swapaxes(right, 1, 2), left_side=True, lower=True)
    mixed = lax.linalg.triangular_solve(root, half, left_side=True, lower=True, transpose_a=True)
    change = jnp.einsum('lir,lrw->liw', left, mixed, precision=lax.Precision.HIGHEST) / REPLICAS
    new_momentum = 0.8 * momentum + change
    new_weights = weights_before - 0.05 * new_momentum
    new_basis = right * lax.rsqrt(lax.optimization_barrier(jnp.mean(right * right, axis=(1, 2), keepdims=True)) + 1e-12)
    return (new_weights, new_basis, new_momentum)
```

```python
import jax
import jax.numpy as jnp
from jax import lax
from jax.experimental import pallas as pl
from jax.experimental.pallas import tpu as pltpu
from jax.sharding import PartitionSpec as P


RANK = 32
LAYERS = 4
LR = LAYERS * RANK
HIGH = lax.Precision.HIGHEST

X_RINGS = [[z * 4 + x for x in range(4)] for z in range(4)]
Z_RINGS = [[z * 4 + x for z in range(4)] for x in range(4)]
CORE_PAIRS = [(j, j ^ 1) for j in range(16)]
CHIP_GROUPS = [[2 * chip + core for chip in range(8)] for core in range(2)]


def hop(rings, step):
    return [(ring[j], ring[(j + step) % len(ring)]) for ring in rings for j in range(len(ring))]


def sum_of_ring(array, axis, rings):
    one, two, three = (lax.ppermute(array, axis, hop(rings, k)) for k in (1, 2, 3))
    return (array + two) + (one + three)


def left_kernel(place, grads, basis, own, one, two, three, total):
    layer = pl.program_id(0)
    small = basis[...].astype(jnp.bfloat16)
    rows = lax.broadcasted_iota(jnp.int32, (LR, small.shape[1]), 0) // RANK
    wide = jnp.where(rows == layer, jnp.concatenate([small] * LAYERS, axis=0), 0)
    part = lax.dot_general(
        grads[...], wide, (((1,), (1,)), ((), ())), preferred_element_type=jnp.float32
    )

    @pl.when(layer == 0)
    def _():
        total[...] = part

    @pl.when(layer > 0)
    def _():
        total[...] += part

    @pl.when(layer == LAYERS - 1)
    def _():
        rows = own.shape[0]
        for step, out in enumerate((own, one, two, three)):
            start = lax.rem(place[0] + step, 4) * rows
            out[...] = total[pl.ds(pl.multiple_of(start, 8), rows), :]


def left_parts(place, grads, basis_t):
    _, layers, rows, width = grads.shape
    piece = jax.ShapeDtypeStruct((rows // 4, LR), jnp.float32)
    return pl.pallas_call(
        left_kernel,
        out_shape=[piece] * 4,
        grid_spec=pltpu.PrefetchScalarGridSpec(
            num_scalar_prefetch=1,
            grid=(layers,),
            in_specs=[
                pl.BlockSpec((None, None, rows, width), lambda l, s: (0, l, 0, 0)),
                pl.BlockSpec((None, RANK, width), lambda l, s: (l, 0, 0)),
            ],
            out_specs=[pl.BlockSpec((rows // 4, LR), lambda l, s: (0, 0))] * 4,
            scratch_shapes=[pltpu.VMEM((rows, LR), jnp.float32)],
        ),
        name="left_parts",
    )(place, grads, basis_t)


def right_kernel(place, grads, own, one, two, three, send, keep, left, small):
    step = pl.program_id(0)

    @pl.when(step == 0)
    def _():
        rows = own.shape[0]
        for back, piece in enumerate((own, one, two, three)):
            start = lax.rem(place[0] + 4 - back, 4) * rows
            left[pl.ds(pl.multiple_of(start, 8), rows), :] = piece[...]
        whole = left[...]
        small[...] = whole.T.astype(jnp.bfloat16)
        full = lax.dot_general(
            whole, whole, (((0,), (0,)), ((), ())), precision=HIGH, preferred_element_type=jnp.float32
        )
        lanes = lax.broadcasted_iota(jnp.int32, (RANK, LR), 1) // RANK
        gram = jnp.zeros((RANK, LR), jnp.float32)
        for l in range(LAYERS):
            gram = jnp.where(lanes == l, full[l * RANK : (l + 1) * RANK, :], gram)
        for out in (send, keep):
            for k in range(4):
                out[64:72, k * LR : (k + 1) * LR] = gram[8 * k : 8 * k + 8, :]
            out[64:72, 4 * LR :] = jnp.zeros((8, out.shape[1] - 4 * LR), jnp.float32)

    layer = lax.rem(step + 2 * (1 - place[1]), 4)
    part = jnp.dot(
        small[pl.ds(pl.multiple_of(layer * RANK, RANK), RANK), :],
        grads[...],
        preferred_element_type=jnp.float32,
    )
    half = pl.multiple_of(lax.rem(step, 2) * RANK, RANK)

    @pl.when(step < 2)
    def _():
        send[pl.ds(half, RANK), :] = part

    @pl.when(step >= 2)
    def _():
        keep[pl.ds(half, RANK), :] = part


def right_parts(place, grads, pieces):
    _, layers, rows, width = grads.shape
    half = jax.ShapeDtypeStruct((LR // 2 + 8, width), jnp.float32)
    whole = lambda l, s: (0, 0)
    return pl.pallas_call(
        right_kernel,
        out_shape=[half, half, jax.ShapeDtypeStruct((rows, LR), jnp.float32)],
        grid_spec=pltpu.PrefetchScalarGridSpec(
            num_scalar_prefetch=1,
            grid=(layers,),
            in_specs=[
                pl.BlockSpec(
                    (None, None, rows, width), lambda l, s: (0, lax.rem(l + 2 * (1 - s[1]), 4), 0, 0)
                )
            ]
            + [pl.BlockSpec((rows // 4, LR), whole)] * 4,
            out_specs=[pl.BlockSpec(half.shape, whole)] * 2 + [pl.BlockSpec((rows, LR), whole)],
            scratch_shapes=[pltpu.VMEM((LR, rows), jnp.bfloat16)],
        ),
        name="right_parts",
    )(place, grads, *pieces)


def inverse_kernel(packed, out):
    gram = jnp.concatenate([packed[:, k * LR : (k + 1) * LR] for k in range(4)], axis=0)
    row = lax.broadcasted_iota(jnp.int32, (RANK, LR), 0)
    lane = lax.broadcasted_iota(jnp.int32, (RANK, LR), 1)
    inner = lane % RANK
    base = lane - inner
    on_diagonal = inner == row
    picked = jnp.sum(jnp.where(on_diagonal, gram, 0.0), axis=0, keepdims=True)
    ridge = jnp.zeros((1, LR), jnp.float32)
    for l in range(LAYERS):
        mine = lane[:1] // RANK == l
        mean = jnp.sum(jnp.where(mine, picked, 0.0), axis=1, keepdims=True) / RANK
        ridge = jnp.where(mine, mean, ridge)
    m = gram + jnp.where(on_diagonal, 0.001 * ridge, 0.0)
    for k in range(RANK):
        column = jnp.take_along_axis(m, base + k, axis=1)
        pivot = 1.0 / column[k : k + 1, :]
        scaled = jnp.where(inner[:1] == k, 1.0, m[k : k + 1, :]) * pivot
        m = jnp.where(row == k, scaled, jnp.where(inner == k, 0.0, m) - column * scaled)
    out[...] = m


def inverses(packed):
    return pl.pallas_call(
        inverse_kernel,
        out_shape=jax.ShapeDtypeStruct((RANK, LR), jnp.float32),
        in_specs=[pl.BlockSpec(memory_space=pltpu.VMEM)],
        out_specs=pl.BlockSpec(memory_space=pltpu.VMEM),
        cost_estimate=pl.CostEstimate(flops=20_000_000, bytes_accessed=32768, transcendentals=0),
        name="inverses",
    )(packed)


def last_kernel(place, replicas, mine, other, left, inverse, weights, momentum, new_w, new_b, new_m):
    core, start = place[1], place[2]
    columns = weights.shape[1]
    width = mine.shape[1]
    for t in range(LAYERS):
        source = mine if t < 2 else other
        layer = 2 * core + t if t < 2 else 2 * (1 - core) + (t - 2)
        right = source[(t % 2) * RANK : (t % 2 + 1) * RANK, :]
        square = jnp.sum(right * right) / (RANK * width)
        new_b[layer] = right * lax.rsqrt(jnp.full((1, 1), square, jnp.float32) + 1e-12)
        turned = pltpu.roll(right, lax.rem(width - start, width), 1)[:, :LR]
        shift = lax.rem(LR - layer * RANK, LR)
        block = pltpu.roll(inverse[...], shift, 1)[:, :RANK]
        mixed = jnp.dot(block, turned, precision=HIGH, preferred_element_type=jnp.float32)
        own = pltpu.roll(left[...], shift, 1)[:, :RANK]
        change = lax.dot_general(
            mixed, own, (((0,), (1,)), ((), ())), precision=HIGH, preferred_element_type=jnp.float32
        )[:columns, :] / replicas
        momentum_now = 0.8 * momentum[layer] + change
        new_m[layer] = momentum_now
        new_w[layer] = weights[layer] - 0.05 * momentum_now


def last_step(place, replicas, mine, other, left, inverse, weights, momentum):
    block = pl.BlockSpec(memory_space=pltpu.VMEM)
    return pl.pallas_call(
        lambda *refs: last_kernel(refs[0], replicas, *refs[1:]),
        out_shape=[
            jax.ShapeDtypeStruct(weights.shape, jnp.float32),
            jax.ShapeDtypeStruct((LAYERS, RANK, mine.shape[1]), jnp.float32),
            jax.ShapeDtypeStruct(weights.shape, jnp.float32),
        ],
        in_specs=[pl.BlockSpec(memory_space=pltpu.SMEM)] + [block] * 6,
        out_specs=[block] * 3,
        name="last_step",
    )(place, mine, other, left, inverse, weights, momentum)


def on_device(gradients, right_factor, weights_before, momentum):
    width = right_factor.shape[1]
    dp, tp = lax.axis_index("dp"), lax.axis_index("tp")
    columns = weights_before.shape[2]
    place = jnp.stack([lax.rem(dp, 4), lax.rem(tp, 2), dp * columns]).astype(jnp.int32)

    own, one, two, three = left_parts(place, gradients, jnp.swapaxes(right_factor, 1, 2))
    one, two, three = (
        lax.ppermute(piece, "dp", hop(X_RINGS, k)) for k, piece in ((1, one), (2, two), (3, three))
    )
    share = sum_of_ring((own + two) + (one + three), "dp", Z_RINGS)
    pieces = [share] + [lax.ppermute(share, "dp", hop(X_RINGS, k)) for k in (1, 2, 3)]

    send, keep, left = right_parts(place, gradients, pieces)
    pair = keep + lax.ppermute(send, "tp", CORE_PAIRS)
    gram = jnp.broadcast_to(pair[None, 64:, : 4 * LR], (8, 8, 4 * LR))
    packet = jnp.concatenate([pair[:64].reshape(8, 8, width), gram], axis=2)
    packet = lax.all_to_all(packet, "tp", 0, 0, tiled=True, axis_index_groups=CHIP_GROUPS)
    packet = jnp.sum(packet, axis=0)
    inverse = inverses(packet[:, width:])
    share = sum_of_ring(packet[:, :width], "dp", X_RINGS)
    share = sum_of_ring(share, "dp", Z_RINGS)
    mine = lax.all_to_all(
        jnp.broadcast_to(share[None], (8, 8, width)), "tp", 0, 0, tiled=True, axis_index_groups=CHIP_GROUPS
    ).reshape(LR // 2, width)
    other = lax.ppermute(mine, "tp", CORE_PAIRS)
    new_w, new_b, new_m = last_step(
        place,
        lax.axis_size("dp"),
        mine,
        other,
        left,
        inverse,
        jnp.swapaxes(weights_before, 1, 2),
        jnp.swapaxes(momentum, 1, 2),
    )
    return tuple(jnp.swapaxes(array, 1, 2) for array in (new_w, new_b, new_m))


def solution(mesh):
    return jax.shard_map(
        on_device,
        mesh=mesh,
        in_specs=(P("dp", None, "tp", None), P(), P(None, "tp", "dp"), P(None, "tp", "dp")),
        out_specs=(P(None, "tp", "dp"), P(), P(None, "tp", "dp")),
        check_vma=False,
    )
```

```python
import jax
import jax.numpy as jnp
from jax import lax
from jax.experimental import pallas as pl
from jax.experimental.pallas import tpu as pltpu
from jax.sharding import PartitionSpec as P


RANK = 32
LAYERS = 4
LR = LAYERS * RANK
HALF = LR // 2
HIGH = lax.Precision.HIGHEST
SMALL = pltpu.CompilerParams(vmem_limit_bytes=16 * 2**20)

X_RINGS = [[z * 4 + x for x in range(4)] for z in range(4)]
Z_RINGS = [[z * 4 + x for z in range(4)] for x in range(4)]
CORE_PAIRS = [(j, j ^ 1) for j in range(16)]
CHIP_GROUPS = [[2 * chip + core for chip in range(8)] for core in range(2)]


def hop(rings, step):
    return [(ring[j], ring[(j + step) % len(ring)]) for ring in rings for j in range(len(ring))]


def to_ring(arrays, rings):
    got = []
    for k, array in enumerate(arrays, 1):
        got.append(lax.ppermute(array, "dp", hop(rings, k)))
    return got


def sum_of_ring(array, rings):
    one, two, three = to_ring([array] * 3, rings)
    return (array + two) + (one + three)


def left_kernel(grads, basis, own, one, two, three, total):
    layer = pl.program_id(0)
    small = basis[...].astype(jnp.bfloat16)
    rows = lax.broadcasted_iota(jnp.int32, (LR, small.shape[1]), 0) // RANK
    wide = jnp.where(rows == layer, jnp.concatenate([small] * LAYERS, axis=0), 0)
    part = lax.dot_general(
        grads[...], wide, (((1,), (1,)), ((), ())), preferred_element_type=jnp.float32
    )

    @pl.when(layer == 0)
    def _():
        total[...] = part

    @pl.when(layer > 0)
    def _():
        total[...] += part

    @pl.when(layer == LAYERS - 1)
    def _():
        rows = own.shape[0]
        x = lax.rem(lax.axis_index("dp"), 4)
        for step, out in enumerate((own, one, two, three)):
            start = lax.rem(x + step, 4) * rows
            out[...] = total[pl.ds(pl.multiple_of(start, 8), rows), :]


def left_parts(grads, basis_t):
    _, layers, rows, width = grads.shape
    piece = jax.ShapeDtypeStruct((rows // 4, LR), jnp.float32)
    return pl.pallas_call(
        left_kernel,
        out_shape=[piece] * 4,
        grid=(layers,),
        in_specs=[
            pl.BlockSpec((None, None, rows, width), lambda l: (0, l, 0, 0)),
            pl.BlockSpec((None, RANK, width), lambda l: (l, 0, 0)),
        ],
        out_specs=[pl.BlockSpec((rows // 4, LR), lambda l: (0, 0))] * 4,
        scratch_shapes=[pltpu.VMEM((rows, LR), jnp.float32)],
        compiler_params=pltpu.CompilerParams(vmem_limit_bytes=54772 * 2**10),
        name="left_parts",
    )(grads, basis_t)


def right_kernel(grads, own, one, two, three, send, keep, left):
    rows = own.shape[0]
    x = lax.rem(lax.axis_index("dp"), 4)
    core = lax.rem(lax.axis_index("tp"), 2)
    for back, piece in enumerate((own, one, two, three)):
        start = lax.rem(x + 4 - back, 4) * rows
        left[pl.ds(pl.multiple_of(start, 8), rows), :] = piece[...]
    whole = left[...]
    small = whole.T.astype(jnp.bfloat16)
    for out, group in ((send, 1 - core), (keep, core)):
        for t in range(2):
            rank = small[t * RANK : (t + 1) * RANK, :]
            other = small[(2 + t) * RANK : (3 + t) * RANK, :]
            out[t * RANK : (t + 1) * RANK, :] = jnp.dot(
                jnp.where(group == 0, rank, other),
                grads[0, 2 * group + t],
                preferred_element_type=jnp.float32,
            )
    full = lax.dot_general(
        whole, whole, (((0,), (0,)), ((), ())), precision=HIGH, preferred_element_type=jnp.float32
    )
    blocks = [full[l * RANK : (l + 1) * RANK, l * RANK : (l + 1) * RANK] for l in range(LAYERS)]
    halves = [jnp.concatenate(blocks[h : h + 2], axis=1) for h in (0, 2)]
    for out, group in ((send, 1 - core), (keep, core)):
        gram = jnp.where(group == 0, halves[0], halves[1])
        for k in range(4):
            out[64:72, k * HALF : (k + 1) * HALF] = gram[8 * k : 8 * k + 8, :]
        out[64:72, 4 * HALF :] = jnp.zeros((8, out.shape[1] - 4 * HALF), jnp.float32)


def right_parts(grads, pieces):
    _, _, rows, width = grads.shape
    half = jax.ShapeDtypeStruct((LR // 2 + 8, width), jnp.float32)
    block = pl.BlockSpec(memory_space=pltpu.VMEM)
    return pl.pallas_call(
        right_kernel,
        out_shape=[half, half, jax.ShapeDtypeStruct((rows, LR), jnp.float32)],
        in_specs=[block] * 5,
        out_specs=[block] * 3,
        compiler_params=SMALL,
        name="right_parts",
    )(grads, *pieces)


def inverse_kernel(packed, out):
    gram = jnp.concatenate([packed[:, k * HALF : (k + 1) * HALF] for k in range(4)], axis=0)
    row = lax.broadcasted_iota(jnp.int32, (RANK, HALF), 0)
    lane = lax.broadcasted_iota(jnp.int32, (RANK, HALF), 1)
    inner = lane % RANK
    on_diagonal = inner == row
    picked = jnp.sum(jnp.where(on_diagonal, gram, 0.0), axis=0, keepdims=True)
    ridge = jnp.zeros((1, HALF), jnp.float32)
    for l in range(2):
        mine = lane[:1] // RANK == l
        mean = jnp.sum(jnp.where(mine, picked, 0.0), axis=1, keepdims=True) / RANK
        ridge = jnp.where(mine, mean, ridge)
    m = gram + jnp.where(on_diagonal, 0.001 * ridge, 0.0)
    for k in range(RANK):
        column = jnp.where(lane < RANK, m[:, k : k + 1], m[:, RANK + k : RANK + k + 1])
        pivot = 1.0 / column[k : k + 1, :]
        scaled = jnp.where(inner[:1] == k, 1.0, m[k : k + 1, :]) * pivot
        m = jnp.where(row == k, scaled, jnp.where(inner == k, 0.0, m) - column * scaled)
    out[...] = m


def inverses(packed):
    return pl.pallas_call(
        inverse_kernel,
        out_shape=jax.ShapeDtypeStruct((RANK, HALF), jnp.float32),
        in_specs=[pl.BlockSpec(memory_space=pltpu.VMEM)],
        out_specs=pl.BlockSpec(memory_space=pltpu.VMEM),
        cost_estimate=pl.CostEstimate(flops=20_000_000, bytes_accessed=32768, transcendentals=0),
        compiler_params=SMALL,
        name="inverses",
    )(packed)


def last_kernel(
    replicas, mine, other, left, mine_inverse, other_inverse, weights, momentum, new_w, new_b, new_m
):
    core = lax.rem(lax.axis_index("tp"), 2)
    columns = weights.shape[1]
    start = lax.axis_index("dp") * columns
    width = mine.shape[1]
    for t in range(LAYERS):
        source, inverse = (mine, mine_inverse) if t < 2 else (other, other_inverse)
        layer = 2 * core + t if t < 2 else 2 * (1 - core) + (t - 2)
        right = source[(t % 2) * RANK : (t % 2 + 1) * RANK, :]
        square = jnp.sum(right * right) / (RANK * width)
        new_b[layer] = right * lax.rsqrt(jnp.full((1, 1), square, jnp.float32) + 1e-12)
        turned = pltpu.roll(right, lax.rem(width - start, width), 1)[:, :LR]
        shift = lax.rem(LR - layer * RANK, LR)
        block = inverse[:, (t % 2) * RANK : (t % 2 + 1) * RANK]
        mixed = jnp.dot(block, turned, precision=HIGH, preferred_element_type=jnp.float32)
        own = pltpu.roll(left[...], shift, 1)[:, :RANK]
        change = lax.dot_general(
            mixed, own, (((0,), (1,)), ((), ())), precision=HIGH, preferred_element_type=jnp.float32
        )[:columns, :] / replicas
        momentum_now = 0.8 * momentum[layer] + change
        new_m[layer] = momentum_now
        new_w[layer] = weights[layer] - 0.05 * momentum_now


def last_step(replicas, mine, other, left, mine_inverse, other_inverse, weights, momentum):
    block = pl.BlockSpec(memory_space=pltpu.VMEM)
    return pl.pallas_call(
        lambda *refs: last_kernel(replicas, *refs),
        out_shape=[
            jax.ShapeDtypeStruct(weights.shape, jnp.float32),
            jax.ShapeDtypeStruct((LAYERS, RANK, mine.shape[1]), jnp.float32),
            jax.ShapeDtypeStruct(weights.shape, jnp.float32),
        ],
        in_specs=[block] * 7,
        out_specs=[block] * 3,
        compiler_params=SMALL,
        name="last_step",
    )(mine, other, left, mine_inverse, other_inverse, weights, momentum)


def one_step(gradients, right_factor, weights_before, momentum):
    width = right_factor.shape[1]
    own, *others = left_parts(gradients, jnp.swapaxes(right_factor, 1, 2))
    one, two, three = to_ring(others, X_RINGS)
    share = sum_of_ring((own + two) + (one + three), Z_RINGS)
    pieces = [share] + to_ring([share] * 3, X_RINGS)

    send, keep, left = right_parts(gradients, pieces)
    pair = keep + lax.ppermute(send, "tp", CORE_PAIRS)
    gram = jnp.broadcast_to(pair[None, 64:, : 4 * HALF], (8, 8, 4 * HALF))
    packet = jnp.concatenate([pair[:64].reshape(8, 8, width), gram], axis=2)
    packet = lax.all_to_all(packet, "tp", 0, 0, tiled=True, axis_index_groups=CHIP_GROUPS)
    packet = jnp.sum(packet, axis=0)
    mine_inverse = inverses(packet[:, width:])
    other_inverse = lax.ppermute(mine_inverse, "tp", CORE_PAIRS)
    share = sum_of_ring(packet[:, :width], X_RINGS)
    share = sum_of_ring(share, Z_RINGS)
    mine = lax.all_to_all(
        jnp.broadcast_to(share[None], (8, 8, width)), "tp", 0, 0, tiled=True, axis_index_groups=CHIP_GROUPS
    ).reshape(HALF, width)
    other = lax.ppermute(mine, "tp", CORE_PAIRS)
    new_w, new_b, new_m = last_step(
        lax.axis_size("dp"),
        mine,
        other,
        left,
        mine_inverse,
        other_inverse,
        jnp.swapaxes(weights_before, 1, 2),
        jnp.swapaxes(momentum, 1, 2),
    )
    return tuple(jnp.swapaxes(array, 1, 2) for array in (new_w, new_b, new_m))


def solution(mesh):
    return jax.shard_map(
        one_step,
        mesh=mesh,
        in_specs=(P("dp", None, "tp", None), P(), P(None, "tp", "dp"), P(None, "tp", "dp")),
        out_specs=(P(None, "tp", "dp"), P(), P(None, "tp", "dp")),
        check_vma=False,
    )
```

```python
import jax
import jax.numpy as jnp
from jax import lax
from jax.experimental import pallas as pl
from jax.experimental.pallas import tpu as pltpu
from jax.sharding import PartitionSpec as P


RANK = 32
LAYERS = 4
LR = LAYERS * RANK
HALF = LR // 2
HIGH = lax.Precision.HIGHEST
SMALL = pltpu.CompilerParams(vmem_limit_bytes=16 * 2**20)

X_RINGS = [[z * 4 + x for x in range(4)] for z in range(4)]
Z_RINGS = [[z * 4 + x for z in range(4)] for x in range(4)]
CORE_PAIRS = [(j, j ^ 1) for j in range(16)]
CHIP_GROUPS = [[2 * chip + core for chip in range(8)] for core in range(2)]


def hop(rings, step):
    return [(ring[j], ring[(j + step) % len(ring)]) for ring in rings for j in range(len(ring))]


def to_ring(arrays, rings):
    got = []
    for k, array in enumerate(arrays, 1):
        got.append(lax.ppermute(array, "dp", hop(rings, k)))
    return got


def sum_of_ring(array, rings):
    one, two, three = to_ring([array] * 3, rings)
    return (array + two) + (one + three)


def left_kernel(grads, basis, own, one, two, three, total_t, total, held, small, sems):
    layers = held.shape[0]
    copies = []
    for l in range(layers):
        copies.append(
            (
                pltpu.make_async_copy(basis.at[l], small.at[l], sems.at[l]),
                pltpu.make_async_copy(grads.at[0, l], held.at[l], sems.at[layers + l]),
            )
        )
    for pair in copies:
        for copy in pair:
            copy.start()
    for l, pair in enumerate(copies):
        for copy in pair:
            copy.wait()
        total_t[l * RANK : (l + 1) * RANK, :] = lax.dot_general(
            small[l].astype(jnp.bfloat16),
            held[l],
            (((1,), (1,)), ((), ())),
            preferred_element_type=jnp.float32,
        )
    total[...] = total_t[...].T
    rows = own.shape[0]
    x = lax.rem(lax.axis_index("dp"), 4)
    for step, out in enumerate((own, one, two, three)):
        start = lax.rem(x + step, 4) * rows
        out[...] = total[pl.ds(pl.multiple_of(start, 8), rows), :]


def left_parts(grads, basis_t):
    _, layers, rows, width = grads.shape
    piece = jax.ShapeDtypeStruct((rows // 4, LR), jnp.float32)
    return pl.pallas_call(
        left_kernel,
        out_shape=[piece] * 4,
        in_specs=[pl.BlockSpec(memory_space=pl.ANY)] * 2,
        out_specs=[pl.BlockSpec(memory_space=pltpu.VMEM)] * 4,
        scratch_shapes=[
            pltpu.VMEM((LR, rows), jnp.float32),
            pltpu.VMEM((rows, LR), jnp.float32),
            pltpu.VMEM((layers, rows, width), jnp.bfloat16),
            pltpu.VMEM((layers, RANK, width), jnp.float32),
            pltpu.SemaphoreType.DMA((2 * layers,)),
        ],
        compiler_params=pltpu.CompilerParams(vmem_limit_bytes=54772 * 2**10),
        name="left_parts",
    )(grads, basis_t)


def right_send_kernel(grads, own, one, two, three, send, keep_gram, keep_small, left):
    rows = own.shape[0]
    x = lax.rem(lax.axis_index("dp"), 4)
    core = lax.rem(lax.axis_index("tp"), 2)
    for back, piece in enumerate((own, one, two, three)):
        start = lax.rem(x + 4 - back, 4) * rows
        left[pl.ds(pl.multiple_of(start, 8), rows), :] = piece[...]
    whole = left[...]
    small = whole.T.astype(jnp.bfloat16)
    low, high = small[:HALF, :], small[HALF:, :]
    keep_small[...] = jnp.where(core == 0, low, high)
    going = jnp.where(core == 0, high, low)
    for t in range(2):
        send[t * RANK : (t + 1) * RANK, :] = jnp.dot(
            going[t * RANK : (t + 1) * RANK, :],
            grads[0, 2 * (1 - core) + t],
            preferred_element_type=jnp.float32,
        )
    full = lax.dot_general(
        whole, whole, (((0,), (0,)), ((), ())), precision=HIGH, preferred_element_type=jnp.float32
    )
    blocks = [full[l * RANK : (l + 1) * RANK, l * RANK : (l + 1) * RANK] for l in range(LAYERS)]
    first, second = (jnp.concatenate(blocks[h : h + 2], axis=1) for h in (0, 2))
    kept = jnp.where(core == 0, first, second)
    gone = jnp.where(core == 0, second, first)
    for k in range(4):
        lanes = slice(k * HALF, (k + 1) * HALF)
        keep_gram[:, lanes] = kept[8 * k : 8 * k + 8, :]
        send[HALF : HALF + 8, lanes] = gone[8 * k : 8 * k + 8, :]
    send[HALF : HALF + 8, 4 * HALF :] = jnp.zeros((8, send.shape[1] - 4 * HALF), jnp.float32)


def right_send(grads, pieces):
    _, _, rows, width = grads.shape
    block = pl.BlockSpec(memory_space=pltpu.VMEM)
    return pl.pallas_call(
        right_send_kernel,
        out_shape=[
            jax.ShapeDtypeStruct((HALF + 8, width), jnp.float32),
            jax.ShapeDtypeStruct((8, 4 * HALF), jnp.float32),
            jax.ShapeDtypeStruct((HALF, rows), jnp.bfloat16),
            jax.ShapeDtypeStruct((rows, LR), jnp.float32),
        ],
        in_specs=[block] * 5,
        out_specs=[block] * 4,
        compiler_params=SMALL,
        name="right_send",
    )(grads, *pieces)


def right_keep_kernel(grads, small, keep):
    core = lax.rem(lax.axis_index("tp"), 2)
    for t in range(2):
        keep[t * RANK : (t + 1) * RANK, :] = jnp.dot(
            small[t * RANK : (t + 1) * RANK, :], grads[0, 2 * core + t], preferred_element_type=jnp.float32
        )


def right_keep(grads, small):
    block = pl.BlockSpec(memory_space=pltpu.VMEM)
    return pl.pallas_call(
        right_keep_kernel,
        out_shape=jax.ShapeDtypeStruct((HALF, grads.shape[3]), jnp.float32),
        in_specs=[block] * 2,
        out_specs=block,
        cost_estimate=pl.CostEstimate(flops=52_000_000, bytes_accessed=2_000_000, transcendentals=0),
        compiler_params=SMALL,
        name="right_keep",
    )(grads, small)


def solve_left(replicas, inverse, left, group, out):
    factor = jnp.where(group == 0, left[:, :HALF], left[:, HALF:])
    for t in range(2):
        lanes = slice(t * RANK, (t + 1) * RANK)
        out[lanes, :] = (
            lax.dot_general(
                inverse[:, lanes],
                factor[:, lanes],
                (((1,), (1,)), ((), ())),
                precision=HIGH,
                preferred_element_type=jnp.float32,
            )
            / replicas
        )


def inverse_kernel(replicas, packed, left, out, factor):
    gram = jnp.concatenate([packed[:, k * HALF : (k + 1) * HALF] for k in range(4)], axis=0)
    row = lax.broadcasted_iota(jnp.int32, (RANK, HALF), 0)
    lane = lax.broadcasted_iota(jnp.int32, (RANK, HALF), 1)
    inner = lane % RANK
    on_diagonal = inner == row
    picked = jnp.sum(jnp.where(on_diagonal, gram, 0.0), axis=0, keepdims=True)
    ridge = jnp.zeros((1, HALF), jnp.float32)
    for l in range(2):
        mine = lane[:1] // RANK == l
        mean = jnp.sum(jnp.where(mine, picked, 0.0), axis=1, keepdims=True) / RANK
        ridge = jnp.where(mine, mean, ridge)
    m = gram + jnp.where(on_diagonal, 0.001 * ridge, 0.0)
    for k in range(RANK):
        column = jnp.where(lane < RANK, m[:, k : k + 1], m[:, RANK + k : RANK + k + 1])
        pivot = 1.0 / column[k : k + 1, :]
        scaled = jnp.where(inner[:1] == k, 1.0, m[k : k + 1, :]) * pivot
        m = jnp.where(row == k, scaled, jnp.where(inner == k, 0.0, m) - column * scaled)
    out[...] = m
    solve_left(replicas, m, left, lax.rem(lax.axis_index("tp"), 2), factor)


def inverses(replicas, packed, left):
    return pl.pallas_call(
        lambda *refs: inverse_kernel(replicas, *refs),
        out_shape=[
            jax.ShapeDtypeStruct((RANK, HALF), jnp.float32),
            jax.ShapeDtypeStruct((HALF, left.shape[0]), jnp.float32),
        ],
        in_specs=[pl.BlockSpec(memory_space=pltpu.VMEM)] * 2,
        out_specs=[pl.BlockSpec(memory_space=pltpu.VMEM)] * 2,
        cost_estimate=pl.CostEstimate(flops=20_000_000, bytes_accessed=32768, transcendentals=0),
        compiler_params=SMALL,
        name="inverses",
    )(packed, left)


def last_kernel(group, right_half, factor, weights, momentum, outs, scratch):
    new_w, new_b, new_m = outs
    buf_w, buf_b, buf_m, sems = scratch
    columns = weights.shape[1]
    width = right_half.shape[1]
    start = lax.axis_index("dp") * columns
    copies = []
    for t in range(2):
        layer = 2 * group + t
        rows = slice(t * RANK, (t + 1) * RANK)
        right = right_half[rows, :]
        turned = pltpu.roll(right, lax.rem(width - start, width), 1)[:, :LR]
        change = lax.dot_general(
            turned,
            factor[rows, :],
            (((0,), (0,)), ((), ())),
            precision=HIGH,
            preferred_element_type=jnp.float32,
        )[:columns, :]
        square = jnp.sum(right * right) / (RANK * width)
        buf_b[t] = right * lax.rsqrt(jnp.full((1, 1), square, jnp.float32) + 1e-12)
        momentum_now = 0.8 * momentum[layer] + change
        buf_m[t] = momentum_now
        buf_w[t] = weights[layer] - 0.05 * momentum_now
        for k, (buf, out) in enumerate(((buf_b, new_b), (buf_m, new_m), (buf_w, new_w))):
            copies.append(pltpu.make_async_copy(buf.at[t], out.at[layer], sems.at[3 * t + k]))
            copies[-1].start()
    return copies


def last_mine_kernel(replicas, right_half, factor, weights, momentum, left, inverse, *refs):
    core = lax.rem(lax.axis_index("tp"), 2)
    copies = last_kernel(core, right_half, factor, weights, momentum, refs[:3], refs[4:])
    solve_left(replicas, inverse, left, 1 - core, refs[3])
    for copy in copies:
        copy.wait()


def last_other_kernel(right_half, factor, weights, momentum, *refs):
    core = lax.rem(lax.axis_index("tp"), 2)
    for copy in last_kernel(1 - core, right_half, factor, weights, momentum, refs[3:6], refs[6:]):
        copy.wait()


def last_half(kernel, right_half, factor, weights, momentum, *, more=(), outs=()):
    block = pl.BlockSpec(memory_space=pltpu.VMEM)
    anywhere = pl.BlockSpec(memory_space=pl.ANY)
    columns, rows = weights.shape[1:]
    width = right_half.shape[1]
    whole = jax.ShapeDtypeStruct(weights.shape, jnp.float32)
    basis = jax.ShapeDtypeStruct((LAYERS, RANK, width), jnp.float32)
    extra = [jax.ShapeDtypeStruct(factor.shape, jnp.float32)] * bool(more)
    return pl.pallas_call(
        kernel,
        out_shape=[whole, basis, whole] + extra,
        in_specs=[block] * (4 + len(more)) + [anywhere] * len(outs),
        out_specs=[anywhere] * 3 + [block] * len(extra),
        scratch_shapes=[
            pltpu.VMEM((2, columns, rows), jnp.float32),
            pltpu.VMEM((2, RANK, width), jnp.float32),
            pltpu.VMEM((2, columns, rows), jnp.float32),
            pltpu.SemaphoreType.DMA((6,)),
        ],
        input_output_aliases={4 + k: k for k in range(len(outs))},
        cost_estimate=pl.CostEstimate(flops=20_000_000, bytes_accessed=1_000_000, transcendentals=0),
        compiler_params=SMALL,
    )(right_half, factor, weights, momentum, *more, *outs)


def one_step(gradients, right_factor, weights_before, momentum):
    width = right_factor.shape[1]
    own, *others = left_parts(gradients, jnp.swapaxes(right_factor, 1, 2))
    one, two, three = to_ring(others, X_RINGS)
    share = sum_of_ring((own + two) + (one + three), Z_RINGS)
    pieces = [share] + to_ring([share] * 3, X_RINGS)

    send, keep_gram, keep_small, left = right_send(gradients, pieces)
    came = lax.ppermute(send, "tp", CORE_PAIRS)
    pair = right_keep(gradients, keep_small) + came[:HALF]
    gram = jnp.broadcast_to((keep_gram + came[HALF:, : 4 * HALF])[None], (8, 8, 4 * HALF))
    packet = jnp.concatenate([pair.reshape(8, 8, width), gram], axis=2)
    packet = lax.all_to_all(packet, "tp", 0, 0, tiled=True, axis_index_groups=CHIP_GROUPS)
    packet = jnp.sum(packet, axis=0)
    replicas = lax.axis_size("dp")
    mine_inverse, mine_factor = inverses(replicas, packet[:, width:], left)
    other_inverse = lax.ppermute(mine_inverse, "tp", CORE_PAIRS)
    share = sum_of_ring(packet[:, :width], X_RINGS)
    share = sum_of_ring(share, Z_RINGS)
    share, other_inverse = lax.optimization_barrier((share, other_inverse))
    mine = lax.all_to_all(
        jnp.broadcast_to(share[None], (8, 8, width)), "tp", 0, 0, tiled=True, axis_index_groups=CHIP_GROUPS
    ).reshape(HALF, width)
    other = lax.ppermute(mine, "tp", CORE_PAIRS)
    state = jnp.swapaxes(weights_before, 1, 2), jnp.swapaxes(momentum, 1, 2)
    *outs, other_factor = last_half(
        lambda *refs: last_mine_kernel(replicas, *refs),
        mine,
        mine_factor,
        *state,
        more=(left, other_inverse),
    )
    outs = last_half(last_other_kernel, other, other_factor, *state, outs=outs)
    return tuple(jnp.swapaxes(array, 1, 2) for array in outs)


def solution(mesh):
    return jax.shard_map(
        one_step,
        mesh=mesh,
        in_specs=(P("dp", None, "tp", None), P(), P(None, "tp", "dp"), P(None, "tp", "dp")),
        out_specs=(P(None, "tp", "dp"), P(), P(None, "tp", "dp")),
        check_vma=False,
    )
```

```python
import jax
import jax.numpy as jnp
from jax import lax
from jax.experimental import pallas as pl
from jax.experimental.pallas import tpu as pltpu
from jax.sharding import PartitionSpec as P


RANK = 32
LAYERS = 4
LR = LAYERS * RANK
HALF = LR // 2
HIGH = lax.Precision.HIGHEST
SMALL = pltpu.CompilerParams(vmem_limit_bytes=16 * 2**20)

X_RINGS = [[z * 4 + x for x in range(4)] for z in range(4)]
Z_RINGS = [[z * 4 + x for z in range(4)] for x in range(4)]
CORE_PAIRS = [(j, j ^ 1) for j in range(16)]
CHIP_GROUPS = [[2 * chip + core for chip in range(8)] for core in range(2)]


def hop(rings, step):
    return [(ring[j], ring[(j + step) % len(ring)]) for ring in rings for j in range(len(ring))]


def to_ring(arrays, rings):
    got = []
    for k, array in enumerate(arrays, 1):
        got.append(lax.ppermute(array, "dp", hop(rings, k)))
    return got


def sum_of_ring(array, rings):
    one, two, three = to_ring([array] * 3, rings)
    return (array + two) + (one + three)


def left_kernel(grads, basis, own, one, two, three, total_t, total, held, small, sems):
    layers = held.shape[0]
    copies = []
    for l in range(layers):
        copies.append(
            (
                pltpu.make_async_copy(basis.at[l], small.at[l], sems.at[l]),
                pltpu.make_async_copy(grads.at[0, l], held.at[l], sems.at[layers + l]),
            )
        )
    for pair in copies:
        for copy in pair:
            copy.start()
    for l, pair in enumerate(copies):
        for copy in pair:
            copy.wait()
        total_t[l * RANK : (l + 1) * RANK, :] = lax.dot_general(
            small[l].astype(jnp.bfloat16),
            held[l],
            (((1,), (1,)), ((), ())),
            preferred_element_type=jnp.float32,
        )
    total[...] = total_t[...].T
    rows = own.shape[0]
    x = lax.rem(lax.axis_index("dp"), 4)
    for step, out in enumerate((own, one, two, three)):
        start = lax.rem(x + step, 4) * rows
        out[...] = total[pl.ds(pl.multiple_of(start, 8), rows), :]


def left_parts(grads, basis_t):
    _, layers, rows, width = grads.shape
    piece = jax.ShapeDtypeStruct((rows // 4, LR), jnp.float32)
    return pl.pallas_call(
        left_kernel,
        out_shape=[piece] * 4,
        in_specs=[pl.BlockSpec(memory_space=pl.ANY)] * 2,
        out_specs=[pl.BlockSpec(memory_space=pltpu.VMEM)] * 4,
        scratch_shapes=[
            pltpu.VMEM((LR, rows), jnp.float32),
            pltpu.VMEM((rows, LR), jnp.float32),
            pltpu.VMEM((layers, rows, width), jnp.bfloat16),
            pltpu.VMEM((layers, RANK, width), jnp.float32),
            pltpu.SemaphoreType.DMA((2 * layers,)),
        ],
        compiler_params=pltpu.CompilerParams(vmem_limit_bytes=54772 * 2**10),
        name="left_parts",
    )(grads, basis_t)


def right_send_kernel(grads, own, one, two, three, send, keep_gram, keep_small, left):
    rows = own.shape[0]
    x = lax.rem(lax.axis_index("dp"), 4)
    core = lax.rem(lax.axis_index("tp"), 2)
    for back, piece in enumerate((own, one, two, three)):
        start = lax.rem(x + 4 - back, 4) * rows
        left[pl.ds(pl.multiple_of(start, 8), rows), :] = piece[...]
    whole = left[...]
    small = whole.T.astype(jnp.bfloat16)
    low, high = small[:HALF, :], small[HALF:, :]
    keep_small[...] = jnp.where(core == 0, low, high)
    going = jnp.where(core == 0, high, low)
    for t in range(2):
        send[t * RANK : (t + 1) * RANK, :] = jnp.dot(
            going[t * RANK : (t + 1) * RANK, :],
            grads[0, 2 * (1 - core) + t],
            preferred_element_type=jnp.float32,
        )
    full = lax.dot_general(
        whole, whole, (((0,), (0,)), ((), ())), precision=HIGH, preferred_element_type=jnp.float32
    )
    blocks = [full[l * RANK : (l + 1) * RANK, l * RANK : (l + 1) * RANK] for l in range(LAYERS)]
    first, second = (jnp.concatenate(blocks[h : h + 2], axis=1) for h in (0, 2))
    kept = jnp.where(core == 0, first, second)
    gone = jnp.where(core == 0, second, first)
    for k in range(4):
        lanes = slice(k * HALF, (k + 1) * HALF)
        keep_gram[:, lanes] = kept[8 * k : 8 * k + 8, :]
        send[HALF : HALF + 8, lanes] = gone[8 * k : 8 * k + 8, :]
    send[HALF : HALF + 8, 4 * HALF :] = jnp.zeros((8, send.shape[1] - 4 * HALF), jnp.float32)


def right_send(grads, pieces):
    _, _, rows, width = grads.shape
    block = pl.BlockSpec(memory_space=pltpu.VMEM)
    return pl.pallas_call(
        right_send_kernel,
        out_shape=[
            jax.ShapeDtypeStruct((HALF + 8, width), jnp.float32),
            jax.ShapeDtypeStruct((8, 4 * HALF), jnp.float32),
            jax.ShapeDtypeStruct((HALF, rows), jnp.bfloat16),
            jax.ShapeDtypeStruct((rows, LR), jnp.float32),
        ],
        in_specs=[block] * 5,
        out_specs=[block] * 4,
        compiler_params=SMALL,
        name="right_send",
    )(grads, *pieces)


def right_keep_kernel(grads, small, keep):
    core = lax.rem(lax.axis_index("tp"), 2)
    for t in range(2):
        keep[t * RANK : (t + 1) * RANK, :] = jnp.dot(
            small[t * RANK : (t + 1) * RANK, :], grads[0, 2 * core + t], preferred_element_type=jnp.float32
        )


def right_keep(grads, small):
    block = pl.BlockSpec(memory_space=pltpu.VMEM)
    return pl.pallas_call(
        right_keep_kernel,
        out_shape=jax.ShapeDtypeStruct((HALF, grads.shape[3]), jnp.float32),
        in_specs=[block] * 2,
        out_specs=block,
        cost_estimate=pl.CostEstimate(flops=52_000_000, bytes_accessed=2_000_000, transcendentals=0),
        compiler_params=SMALL,
        name="right_keep",
    )(grads, small)


def solve_left(replicas, inverse, left, group, out):
    factor = jnp.where(group == 0, left[:, :HALF], left[:, HALF:])
    for t in range(2):
        lanes = slice(t * RANK, (t + 1) * RANK)
        out[lanes, :] = (
            lax.dot_general(
                inverse[:, lanes],
                factor[:, lanes],
                (((1,), (1,)), ((), ())),
                precision=HIGH,
                preferred_element_type=jnp.float32,
            )
            / replicas
        )


def inverse_kernel(replicas, packed, left, out, factor):
    gram = jnp.concatenate([packed[:, k * HALF : (k + 1) * HALF] for k in range(4)], axis=0)
    row = lax.broadcasted_iota(jnp.int32, (RANK, HALF), 0)
    lane = lax.broadcasted_iota(jnp.int32, (RANK, HALF), 1)
    inner = lane % RANK
    on_diagonal = inner == row
    picked = jnp.sum(jnp.where(on_diagonal, gram, 0.0), axis=0, keepdims=True)
    ridge = jnp.zeros((1, HALF), jnp.float32)
    for l in range(2):
        mine = lane[:1] // RANK == l
        mean = jnp.sum(jnp.where(mine, picked, 0.0), axis=1, keepdims=True) / RANK
        ridge = jnp.where(mine, mean, ridge)
    m = gram + jnp.where(on_diagonal, 0.001 * ridge, 0.0)
    for k in range(RANK):
        column = jnp.where(lane < RANK, m[:, k : k + 1], m[:, RANK + k : RANK + k + 1])
        pivot = 1.0 / column[k : k + 1, :]
        scaled = jnp.where(inner[:1] == k, 1.0, m[k : k + 1, :]) * pivot
        m = jnp.where(row == k, scaled, jnp.where(inner == k, 0.0, m) - column * scaled)
    out[...] = m
    solve_left(replicas, m, left, lax.rem(lax.axis_index("tp"), 2), factor)


def inverses(replicas, packed, left):
    return pl.pallas_call(
        lambda *refs: inverse_kernel(replicas, *refs),
        out_shape=[
            jax.ShapeDtypeStruct((RANK, HALF), jnp.float32),
            jax.ShapeDtypeStruct((HALF, left.shape[0]), jnp.float32),
        ],
        in_specs=[pl.BlockSpec(memory_space=pltpu.VMEM)] * 2,
        out_specs=[pl.BlockSpec(memory_space=pltpu.VMEM)] * 2,
        cost_estimate=pl.CostEstimate(flops=20_000_000, bytes_accessed=32768, transcendentals=0),
        compiler_params=SMALL,
        name="inverses",
    )(packed, left)


def last_kernel(group, right_half, factor, weights, momentum, outs, scratch):
    new_w, new_b, new_m = outs
    buf_w, buf_b, buf_m, sems = scratch
    columns = weights.shape[1]
    width = right_half.shape[1]
    start = lax.axis_index("dp") * columns
    copies = []
    for t in range(2):
        layer = 2 * group + t
        rows = slice(t * RANK, (t + 1) * RANK)
        right = right_half[rows, :]
        turned = pltpu.roll(right, lax.rem(width - start, width), 1)[:, :LR]
        change = lax.dot_general(
            turned,
            factor[rows, :],
            (((0,), (0,)), ((), ())),
            precision=HIGH,
            preferred_element_type=jnp.float32,
        )[:columns, :]
        square = jnp.sum(right * right) / (RANK * width)
        buf_b[t] = right * lax.rsqrt(jnp.full((1, 1), square, jnp.float32) + 1e-12)
        momentum_now = 0.8 * momentum[layer] + change
        buf_m[t] = momentum_now
        buf_w[t] = weights[layer] - 0.05 * momentum_now
        for k, (buf, out) in enumerate(((buf_b, new_b), (buf_m, new_m), (buf_w, new_w))):
            copies.append(pltpu.make_async_copy(buf.at[t], out.at[layer], sems.at[3 * t + k]))
            copies[-1].start()
    return copies


def last_mine_kernel(right_half, factor, weights, momentum, *refs):
    core = lax.rem(lax.axis_index("tp"), 2)
    for copy in last_kernel(core, right_half, factor, weights, momentum, refs[:3], refs[3:]):
        copy.wait()


def last_other_kernel(replicas, right_half, inverse, weights, momentum, left, *refs):
    other = 1 - lax.rem(lax.axis_index("tp"), 2)
    factor = refs[-1]
    solve_left(replicas, inverse, left, other, factor)
    for copy in last_kernel(other, right_half, factor, weights, momentum, refs[3:6], refs[6:-1]):
        copy.wait()


def last_half(kernel, right_half, factor, weights, momentum, *, more=(), outs=()):
    block = pl.BlockSpec(memory_space=pltpu.VMEM)
    anywhere = pl.BlockSpec(memory_space=pl.ANY)
    columns, rows = weights.shape[1:]
    width = right_half.shape[1]
    whole = jax.ShapeDtypeStruct(weights.shape, jnp.float32)
    basis = jax.ShapeDtypeStruct((LAYERS, RANK, width), jnp.float32)
    extra = [pltpu.VMEM((HALF, rows), jnp.float32)] * bool(more)
    return pl.pallas_call(
        kernel,
        out_shape=[whole, basis, whole],
        in_specs=[block] * (4 + len(more)) + [anywhere] * len(outs),
        out_specs=[anywhere] * 3,
        scratch_shapes=[
            pltpu.VMEM((2, columns, rows), jnp.float32),
            pltpu.VMEM((2, RANK, width), jnp.float32),
            pltpu.VMEM((2, columns, rows), jnp.float32),
            pltpu.SemaphoreType.DMA((6,)),
        ]
        + extra,
        input_output_aliases={4 + len(more) + k: k for k in range(len(outs))},
        cost_estimate=pl.CostEstimate(flops=20_000_000, bytes_accessed=1_000_000, transcendentals=0),
        compiler_params=SMALL,
    )(right_half, factor, weights, momentum, *more, *outs)


def one_step(gradients, right_factor, weights_before, momentum):
    width = right_factor.shape[1]
    own, *others = left_parts(gradients, jnp.swapaxes(right_factor, 1, 2))
    one, two, three = to_ring(others, X_RINGS)
    share = sum_of_ring((own + two) + (one + three), Z_RINGS)
    pieces = [share] + to_ring([share] * 3, X_RINGS)

    send, keep_gram, keep_small, left = right_send(gradients, pieces)
    came = lax.ppermute(send, "tp", CORE_PAIRS)
    pair = right_keep(gradients, keep_small) + came[:HALF]
    gram = jnp.broadcast_to((keep_gram + came[HALF:, : 4 * HALF])[None], (8, 8, 4 * HALF))
    packet = jnp.concatenate([pair.reshape(8, 8, width), gram], axis=2)
    packet = lax.all_to_all(packet, "tp", 0, 0, tiled=True, axis_index_groups=CHIP_GROUPS)
    packet = jnp.sum(packet, axis=0)
    replicas = lax.axis_size("dp")
    mine_inverse, mine_factor = inverses(replicas, packet[:, width:], left)
    share = sum_of_ring(packet[:, :width], X_RINGS)
    share = sum_of_ring(share, Z_RINGS)
    mine = lax.all_to_all(
        jnp.broadcast_to(share[None], (8, 8, width)), "tp", 0, 0, tiled=True, axis_index_groups=CHIP_GROUPS
    ).reshape(HALF, width)
    other = lax.ppermute(mine, "tp", CORE_PAIRS)
    other_inverse = lax.ppermute(mine_inverse, "tp", CORE_PAIRS)
    state = jnp.swapaxes(weights_before, 1, 2), jnp.swapaxes(momentum, 1, 2)
    outs = last_half(last_mine_kernel, mine, mine_factor, *state)
    outs = last_half(
        lambda *refs: last_other_kernel(replicas, *refs),
        other,
        other_inverse,
        *state,
        more=(left,),
        outs=outs,
    )
    return tuple(jnp.swapaxes(array, 1, 2) for array in outs)


def solution(mesh):
    return jax.shard_map(
        one_step,
        mesh=mesh,
        in_specs=(P("dp", None, "tp", None), P(), P(None, "tp", "dp"), P(None, "tp", "dp")),
        out_specs=(P(None, "tp", "dp"), P(), P(None, "tp", "dp")),
        check_vma=False,
    )
```

```python
import jax
import jax.numpy as jnp
from jax import lax
from jax.experimental import pallas as pl
from jax.experimental.pallas import tpu as pltpu
from jax.sharding import PartitionSpec as P


RANK = 32
LAYERS = 4
LR = LAYERS * RANK
HALF = LR // 2
HIGH = lax.Precision.HIGHEST
SMALL = pltpu.CompilerParams(vmem_limit_bytes=16 * 2**20)

X_RINGS = [[z * 4 + x for x in range(4)] for z in range(4)]
Z_RINGS = [[z * 4 + x for z in range(4)] for x in range(4)]
CORE_PAIRS = [(j, j ^ 1) for j in range(16)]
CHIP_GROUPS = [[2 * chip + core for chip in range(8)] for core in range(2)]


def hop(rings, step):
    return [(ring[j], ring[(j + step) % len(ring)]) for ring in rings for j in range(len(ring))]


def to_ring(arrays, rings):
    got = []
    for k, array in enumerate(arrays, 1):
        got.append(lax.ppermute(array, "dp", hop(rings, k)))
    return got


def sum_of_ring(array, rings):
    one, two, three = to_ring([array] * 3, rings)
    return (array + two) + (one + three)


def left_kernel(grads, basis, own, one, two, three, total_t, total):
    step = pl.program_id(0)
    layers = grads.shape[0]
    for l in range(layers):
        start = pl.multiple_of((step * layers + l) * RANK, RANK)
        total_t[pl.ds(start, RANK), :] = lax.dot_general(
            basis[l].astype(jnp.bfloat16), grads[l], (((1,), (1,)), ((), ())), preferred_element_type=jnp.float32
        )

    @pl.when(step == pl.num_programs(0) - 1)
    def _():
        total[...] = total_t[...].T
        rows = own.shape[0]
        x = lax.rem(lax.axis_index("dp"), 4)
        for back, out in enumerate((own, one, two, three)):
            start = lax.rem(x + back, 4) * rows
            out[...] = total[pl.ds(pl.multiple_of(start, 8), rows), :]


def left_parts(grads, basis_t):
    _, layers, rows, width = grads.shape
    piece = jax.ShapeDtypeStruct((rows // 4, LR), jnp.float32)
    return pl.pallas_call(
        left_kernel,
        out_shape=[piece] * 4,
        grid=(2,),
        in_specs=[
            pl.BlockSpec((None, layers // 2, rows, width), lambda l: (0, l, 0, 0)),
            pl.BlockSpec((layers // 2, RANK, width), lambda l: (l, 0, 0)),
        ],
        out_specs=[pl.BlockSpec((rows // 4, LR), lambda l: (0, 0))] * 4,
        scratch_shapes=[pltpu.VMEM((LR, rows), jnp.float32), pltpu.VMEM((rows, LR), jnp.float32)],
        compiler_params=pltpu.CompilerParams(vmem_limit_bytes=54772 * 2**10),
        name="left_parts",
    )(grads, basis_t)


def right_send_kernel(grads, own, one, two, three, send, keep_gram, keep_small, left):
    rows = own.shape[0]
    x = lax.rem(lax.axis_index("dp"), 4)
    core = lax.rem(lax.axis_index("tp"), 2)
    for back, piece in enumerate((own, one, two, three)):
        start = lax.rem(x + 4 - back, 4) * rows
        left[pl.ds(pl.multiple_of(start, 8), rows), :] = piece[...]
    whole = left[...]
    small = whole.T.astype(jnp.bfloat16)
    low, high = small[:HALF, :], small[HALF:, :]
    keep_small[...] = jnp.where(core == 0, low, high)
    going = jnp.where(core == 0, high, low)
    for t in range(2):
        send[t * RANK : (t + 1) * RANK, :] = jnp.dot(
            going[t * RANK : (t + 1) * RANK, :],
            grads[0, 2 * (1 - core) + t],
            preferred_element_type=jnp.float32,
        )
    full = lax.dot_general(
        whole, whole, (((0,), (0,)), ((), ())), precision=HIGH, preferred_element_type=jnp.float32
    )
    blocks = [full[l * RANK : (l + 1) * RANK, l * RANK : (l + 1) * RANK] for l in range(LAYERS)]
    first, second = (jnp.concatenate(blocks[h : h + 2], axis=1) for h in (0, 2))
    kept = jnp.where(core == 0, first, second)
    gone = jnp.where(core == 0, second, first)
    for k in range(4):
        lanes = slice(k * HALF, (k + 1) * HALF)
        keep_gram[:, lanes] = kept[8 * k : 8 * k + 8, :]
        send[HALF : HALF + 8, lanes] = gone[8 * k : 8 * k + 8, :]
    send[HALF : HALF + 8, 4 * HALF :] = jnp.zeros((8, send.shape[1] - 4 * HALF), jnp.float32)


def right_send(grads, pieces):
    _, _, rows, width = grads.shape
    block = pl.BlockSpec(memory_space=pltpu.VMEM)
    return pl.pallas_call(
        right_send_kernel,
        out_shape=[
            jax.ShapeDtypeStruct((HALF + 8, width), jnp.float32),
            jax.ShapeDtypeStruct((8, 4 * HALF), jnp.float32),
            jax.ShapeDtypeStruct((HALF, rows), jnp.bfloat16),
            jax.ShapeDtypeStruct((rows, LR), jnp.float32),
        ],
        in_specs=[block] * 5,
        out_specs=[block] * 4,
        compiler_params=SMALL,
        name="right_send",
    )(grads, *pieces)


def right_keep_kernel(grads, small, keep):
    core = lax.rem(lax.axis_index("tp"), 2)
    for t in range(2):
        keep[t * RANK : (t + 1) * RANK, :] = jnp.dot(
            small[t * RANK : (t + 1) * RANK, :], grads[0, 2 * core + t], preferred_element_type=jnp.float32
        )


def right_keep(grads, small):
    block = pl.BlockSpec(memory_space=pltpu.VMEM)
    return pl.pallas_call(
        right_keep_kernel,
        out_shape=jax.ShapeDtypeStruct((HALF, grads.shape[3]), jnp.float32),
        in_specs=[block] * 2,
        out_specs=block,
        cost_estimate=pl.CostEstimate(flops=52_000_000, bytes_accessed=2_000_000, transcendentals=0),
        compiler_params=SMALL,
        name="right_keep",
    )(grads, small)


def unpacked(packed):
    return jnp.concatenate([packed[:, k * HALF : (k + 1) * HALF] for k in range(4)], axis=0)


def solve_left(replicas, inverse, left, group, out):
    factor = jnp.where(group == 0, left[:, :HALF], left[:, HALF:])
    for t in range(2):
        lanes = slice(t * RANK, (t + 1) * RANK)
        out[lanes, :] = (
            lax.dot_general(
                inverse[:, lanes],
                factor[:, lanes],
                (((1,), (1,)), ((), ())),
                precision=HIGH,
                preferred_element_type=jnp.float32,
            )
            / replicas
        )


def inverse_kernel(replicas, packed, left, out, factor):
    gram = unpacked(packed)
    row = lax.broadcasted_iota(jnp.int32, (RANK, HALF), 0)
    lane = lax.broadcasted_iota(jnp.int32, (RANK, HALF), 1)
    inner = lane % RANK
    on_diagonal = inner == row
    picked = jnp.sum(jnp.where(on_diagonal, gram, 0.0), axis=0, keepdims=True)
    ridge = jnp.zeros((1, HALF), jnp.float32)
    for l in range(2):
        mine = lane[:1] // RANK == l
        mean = jnp.sum(jnp.where(mine, picked, 0.0), axis=1, keepdims=True) / RANK
        ridge = jnp.where(mine, mean, ridge)
    m = gram + jnp.where(on_diagonal, 0.001 * ridge, 0.0)
    for k in range(RANK):
        column = jnp.where(lane < RANK, m[:, k : k + 1], m[:, RANK + k : RANK + k + 1])
        pivot = 1.0 / column[k : k + 1, :]
        scaled = jnp.where(inner[:1] == k, 1.0, m[k : k + 1, :]) * pivot
        m = jnp.where(row == k, scaled, jnp.where(inner == k, 0.0, m) - column * scaled)
    for k in range(4):
        out[:, k * HALF : (k + 1) * HALF] = m[8 * k : 8 * k + 8, :]
    solve_left(replicas, m, left, lax.rem(lax.axis_index("tp"), 2), factor)


def inverses(replicas, packed, left):
    return pl.pallas_call(
        lambda *refs: inverse_kernel(replicas, *refs),
        out_shape=[
            jax.ShapeDtypeStruct((8, 4 * HALF), jnp.float32),
            jax.ShapeDtypeStruct((HALF, left.shape[0]), jnp.float32),
        ],
        in_specs=[pl.BlockSpec(memory_space=pltpu.VMEM)] * 2,
        out_specs=[pl.BlockSpec(memory_space=pltpu.VMEM)] * 2,
        cost_estimate=pl.CostEstimate(flops=20_000_000, bytes_accessed=32768, transcendentals=0),
        compiler_params=SMALL,
        name="inverses",
    )(packed, left)


def last_kernel(group, right_half, factor, weights, momentum, outs, scratch):
    new_w, new_b, new_m = outs
    buf_w, buf_b, buf_m, sems = scratch
    columns = weights.shape[1]
    width = right_half.shape[1]
    start = lax.axis_index("dp") * columns
    copies = []
    for t in range(2):
        layer = 2 * group + t
        rows = slice(t * RANK, (t + 1) * RANK)
        right = right_half[rows, :]
        turned = pltpu.roll(right, lax.rem(width - start, width), 1)[:, :LR]
        change = lax.dot_general(
            turned,
            factor[rows, :],
            (((0,), (0,)), ((), ())),
            precision=HIGH,
            preferred_element_type=jnp.float32,
        )[:columns, :]
        square = jnp.sum(right * right) / (RANK * width)
        buf_b[t] = right * lax.rsqrt(jnp.full((1, 1), square, jnp.float32) + 1e-12)
        momentum_now = 0.8 * momentum[layer] + change
        buf_m[t] = momentum_now
        buf_w[t] = weights[layer] - 0.05 * momentum_now
        for k, (buf, out) in enumerate(((buf_b, new_b), (buf_m, new_m), (buf_w, new_w))):
            copies.append(pltpu.make_async_copy(buf.at[t], out.at[layer], sems.at[3 * t + k]))
            copies[-1].start()
    return copies


def last_mine_kernel(right_half, factor, weights, momentum, *refs):
    core = lax.rem(lax.axis_index("tp"), 2)
    for copy in last_kernel(core, right_half, factor, weights, momentum, refs[:3], refs[3:]):
        copy.wait()


def last_other_kernel(replicas, right_half, left, weights, momentum, *refs):
    other = 1 - lax.rem(lax.axis_index("tp"), 2)
    factor = refs[-1]
    solve_left(replicas, unpacked(right_half[HALF:, : 4 * HALF]), left, other, factor)
    for copy in last_kernel(other, right_half, factor, weights, momentum, refs[3:6], refs[6:-1]):
        copy.wait()


def last_half(kernel, right_half, factor, weights, momentum, outs=()):
    block = pl.BlockSpec(memory_space=pltpu.VMEM)
    anywhere = pl.BlockSpec(memory_space=pl.ANY)
    columns, rows = weights.shape[1:]
    width = right_half.shape[1]
    whole = jax.ShapeDtypeStruct(weights.shape, jnp.float32)
    basis = jax.ShapeDtypeStruct((LAYERS, RANK, width), jnp.float32)
    extra = [pltpu.VMEM((HALF, rows), jnp.float32)] * bool(outs)
    return pl.pallas_call(
        kernel,
        out_shape=[whole, basis, whole],
        in_specs=[block] * 4 + [anywhere] * len(outs),
        out_specs=[anywhere] * 3,
        scratch_shapes=[
            pltpu.VMEM((2, columns, rows), jnp.float32),
            pltpu.VMEM((2, RANK, width), jnp.float32),
            pltpu.VMEM((2, columns, rows), jnp.float32),
            pltpu.SemaphoreType.DMA((6,)),
        ]
        + extra,
        input_output_aliases={4 + k: k for k in range(len(outs))},
        cost_estimate=pl.CostEstimate(flops=20_000_000, bytes_accessed=1_000_000, transcendentals=0),
        compiler_params=SMALL,
    )(right_half, factor, weights, momentum, *outs)


def one_step(gradients, right_factor, weights_before, momentum):
    width = right_factor.shape[1]
    own, *others = left_parts(gradients, jnp.swapaxes(right_factor, 1, 2))
    one, two, three = to_ring(others, X_RINGS)
    share = sum_of_ring((own + two) + (one + three), Z_RINGS)
    pieces = [share] + to_ring([share] * 3, X_RINGS)

    send, keep_gram, keep_small, left = right_send(gradients, pieces)
    came = lax.ppermute(send, "tp", CORE_PAIRS)
    pair = right_keep(gradients, keep_small) + came[:HALF]
    gram = jnp.broadcast_to((keep_gram + came[HALF:, : 4 * HALF])[None], (8, 8, 4 * HALF))
    packet = jnp.concatenate([pair.reshape(8, 8, width), gram], axis=2)
    packet = lax.all_to_all(packet, "tp", 0, 0, tiled=True, axis_index_groups=CHIP_GROUPS)
    packet = jnp.sum(packet, axis=0)
    replicas = lax.axis_size("dp")
    mine_inverse, mine_factor = inverses(replicas, packet[:, width:], left)
    share = sum_of_ring(packet[:, :width], X_RINGS)
    share = sum_of_ring(share, Z_RINGS)
    mine = lax.all_to_all(
        jnp.broadcast_to(share[None], (8, 8, width)), "tp", 0, 0, tiled=True, axis_index_groups=CHIP_GROUPS
    ).reshape(HALF, width)
    going = jnp.concatenate([mine, jnp.pad(mine_inverse, ((0, 0), (0, width - 4 * HALF)))], axis=0)
    other = lax.ppermute(going, "tp", CORE_PAIRS)
    state = jnp.swapaxes(weights_before, 1, 2), jnp.swapaxes(momentum, 1, 2)
    outs = last_half(last_mine_kernel, mine, mine_factor, *state)
    outs = last_half(lambda *refs: last_other_kernel(replicas, *refs), other, left, *state, outs)
    return tuple(jnp.swapaxes(array, 1, 2) for array in outs)


def solution(mesh):
    return jax.shard_map(
        one_step,
        mesh=mesh,
        in_specs=(P("dp", None, "tp", None), P(), P(None, "tp", "dp"), P(None, "tp", "dp")),
        out_specs=(P(None, "tp", "dp"), P(), P(None, "tp", "dp")),
        check_vma=False,
    )
```

```python
import jax
import jax.numpy as jnp
from jax import lax
from jax.experimental import pallas as pl
from jax.experimental.pallas import tpu as pltpu
from jax.sharding import PartitionSpec as P


RANK = 32
LAYERS = 4
LR = LAYERS * RANK
HALF = LR // 2
HIGH = lax.Precision.HIGHEST
SMALL = pltpu.CompilerParams(vmem_limit_bytes=16 * 2**20)

X_RINGS = [[z * 4 + x for x in range(4)] for z in range(4)]
Z_RINGS = [[z * 4 + x for z in range(4)] for x in range(4)]
CORE_PAIRS = [(j, j ^ 1) for j in range(16)]
CHIP_GROUPS = [[2 * chip + core for chip in range(8)] for core in range(2)]


def hop(rings, step):
    return [(ring[j], ring[(j + step) % len(ring)]) for ring in rings for j in range(len(ring))]


def to_ring(arrays, rings):
    got = []
    for k, array in enumerate(arrays, 1):
        got.append(lax.ppermute(array, "dp", hop(rings, k)))
    return got


def sum_of_ring(array, rings):
    one, two, three = to_ring([array] * 3, rings)
    return (array + two) + (one + three)


def left_kernel(grads, basis, own, one, two, three, total_t, total):
    step = pl.program_id(0)
    layers = grads.shape[0]
    for l in range(layers):
        start = pl.multiple_of((step * layers + l) * RANK, RANK)
        total_t[pl.ds(start, RANK), :] = lax.dot_general(
            basis[l].astype(jnp.bfloat16), grads[l], (((1,), (1,)), ((), ())), preferred_element_type=jnp.float32
        )

    @pl.when(step == pl.num_programs(0) - 1)
    def _():
        total[...] = total_t[...].T
        rows = own.shape[0]
        x = lax.rem(lax.axis_index("dp"), 4)
        for back, out in enumerate((own, one, two, three)):
            start = lax.rem(x + back, 4) * rows
            out[...] = total[pl.ds(pl.multiple_of(start, 8), rows), :]


def left_parts(grads, basis_t):
    _, layers, rows, width = grads.shape
    piece = jax.ShapeDtypeStruct((rows // 4, LR), jnp.float32)
    return pl.pallas_call(
        left_kernel,
        out_shape=[piece] * 4,
        grid=(2,),
        in_specs=[
            pl.BlockSpec((None, layers // 2, rows, width), lambda l: (0, l, 0, 0)),
            pl.BlockSpec((layers // 2, RANK, width), lambda l: (l, 0, 0)),
        ],
        out_specs=[pl.BlockSpec((rows // 4, LR), lambda l: (0, 0))] * 4,
        scratch_shapes=[pltpu.VMEM((LR, rows), jnp.float32), pltpu.VMEM((rows, LR), jnp.float32)],
        compiler_params=pltpu.CompilerParams(vmem_limit_bytes=54772 * 2**10),
        name="left_parts",
    )(grads, basis_t)


def right_send_kernel(grads, own, one, two, three, send, keep_gram, keep_small, left):
    rows = own.shape[0]
    x = lax.rem(lax.axis_index("dp"), 4)
    core = lax.rem(lax.axis_index("tp"), 2)
    for back, piece in enumerate((own, one, two, three)):
        start = lax.rem(x + 4 - back, 4) * rows
        left[pl.ds(pl.multiple_of(start, 8), rows), :] = piece[...]
    whole = left[...]
    small = whole.T.astype(jnp.bfloat16)
    low, high = small[:HALF, :], small[HALF:, :]
    keep_small[...] = jnp.where(core == 0, low, high)
    going = jnp.where(core == 0, high, low)
    for t in range(2):
        send[t * RANK : (t + 1) * RANK, :] = jnp.dot(
            going[t * RANK : (t + 1) * RANK, :],
            grads[0, 2 * (1 - core) + t],
            preferred_element_type=jnp.float32,
        )
    full = lax.dot_general(
        whole, whole, (((0,), (0,)), ((), ())), precision=HIGH, preferred_element_type=jnp.float32
    )
    blocks = [full[l * RANK : (l + 1) * RANK, l * RANK : (l + 1) * RANK] for l in range(LAYERS)]
    first, second = (jnp.concatenate(blocks[h : h + 2], axis=1) for h in (0, 2))
    kept = jnp.where(core == 0, first, second)
    gone = jnp.where(core == 0, second, first)
    for k in range(4):
        lanes = slice(k * HALF, (k + 1) * HALF)
        keep_gram[:, lanes] = kept[8 * k : 8 * k + 8, :]
        send[HALF : HALF + 8, lanes] = gone[8 * k : 8 * k + 8, :]
    send[HALF : HALF + 8, 4 * HALF :] = jnp.zeros((8, send.shape[1] - 4 * HALF), jnp.float32)


def right_send(grads, pieces):
    _, _, rows, width = grads.shape
    block = pl.BlockSpec(memory_space=pltpu.VMEM)
    return pl.pallas_call(
        right_send_kernel,
        out_shape=[
            jax.ShapeDtypeStruct((HALF + 8, width), jnp.float32),
            jax.ShapeDtypeStruct((8, 4 * HALF), jnp.float32),
            jax.ShapeDtypeStruct((HALF, rows), jnp.bfloat16),
            jax.ShapeDtypeStruct((rows, LR), jnp.float32),
        ],
        in_specs=[block] * 5,
        out_specs=[block] * 4,
        compiler_params=SMALL,
        name="right_send",
    )(grads, *pieces)


def right_keep_kernel(grads, small, keep):
    core = lax.rem(lax.axis_index("tp"), 2)
    for t in range(2):
        keep[t * RANK : (t + 1) * RANK, :] = jnp.dot(
            small[t * RANK : (t + 1) * RANK, :], grads[0, 2 * core + t], preferred_element_type=jnp.float32
        )


def right_keep(grads, small):
    block = pl.BlockSpec(memory_space=pltpu.VMEM)
    return pl.pallas_call(
        right_keep_kernel,
        out_shape=jax.ShapeDtypeStruct((HALF, grads.shape[3]), jnp.float32),
        in_specs=[block] * 2,
        out_specs=block,
        cost_estimate=pl.CostEstimate(flops=52_000_000, bytes_accessed=2_000_000, transcendentals=0),
        compiler_params=SMALL,
        name="right_keep",
    )(grads, small)


def unpacked(packed):
    return jnp.concatenate([packed[:, k * HALF : (k + 1) * HALF] for k in range(4)], axis=0)


def solve_left(replicas, root, left, group, out):
    factor = jnp.where(group == 0, left[:, :HALF], left[:, HALF:])
    for t in range(2):
        lanes = slice(t * RANK, (t + 1) * RANK)
        out[lanes, :] = (
            lax.dot_general(
                root[:, lanes],
                factor[:, lanes],
                (((1,), (1,)), ((), ())),
                precision=HIGH,
                preferred_element_type=jnp.float32,
            )
            / replicas
        )


def root_kernel(replicas, packed, left, out, factor):
    gram = unpacked(packed)
    row = lax.broadcasted_iota(jnp.int32, (RANK, LR), 0)
    lane = lax.broadcasted_iota(jnp.int32, (RANK, LR), 1)
    first = (lane // RANK) % 2 == 0
    one = jnp.where(lane % RANK == row, 1.0, 0.0)
    ridge = jnp.zeros((RANK, HALF), jnp.float32)
    for l in range(2):
        mine = lane[:, :HALF] // RANK == l
        on_diagonal = mine & (lane[:, :HALF] % RANK == row[:, :HALF])
        mean = jnp.sum(jnp.where(on_diagonal, gram, 0.0)) / RANK
        ridge = jnp.where(on_diagonal, 0.001 * mean, ridge)
    m = jnp.concatenate([gram + ridge, one[:, HALF:]], axis=1)
    for k in range(RANK - 1):
        column = jnp.where(first, m[:, k : k + 1], m[:, RANK + k : RANK + k + 1])
        scale = jnp.where(row > k, column * (1.0 / column[k : k + 1, :]), 0.0)
        m = m - scale * m[k : k + 1, :]
    pivots = [
        jnp.sum(jnp.where(lane == row + l * RANK, m, 0.0), axis=1, keepdims=True) for l in range(2)
    ]
    pivot = jnp.where(first, pivots[0], pivots[1])[:, HALF:]
    shrink = lax.rsqrt(pivot)
    shrink = shrink * (1.5 - 0.5 * (pivot * shrink) * shrink)
    root = m[:, HALF:] * shrink
    for k in range(4):
        out[:, k * HALF : (k + 1) * HALF] = root[8 * k : 8 * k + 8, :]
    solve_left(replicas, root, left, lax.rem(lax.axis_index("tp"), 2), factor)


def inverse_roots(replicas, packed, left):
    return pl.pallas_call(
        lambda *refs: root_kernel(replicas, *refs),
        out_shape=[
            jax.ShapeDtypeStruct((8, 4 * HALF), jnp.float32),
            jax.ShapeDtypeStruct((HALF, left.shape[0]), jnp.float32),
        ],
        in_specs=[pl.BlockSpec(memory_space=pltpu.VMEM)] * 2,
        out_specs=[pl.BlockSpec(memory_space=pltpu.VMEM)] * 2,
        cost_estimate=pl.CostEstimate(flops=20_000_000, bytes_accessed=32768, transcendentals=0),
        compiler_params=SMALL,
        name="inverse_roots",
    )(packed, left)


def last_kernel(group, right_half, root, factor, weights, momentum, outs, scratch):
    new_w, new_b, new_m = outs
    buf_w, buf_b, buf_m, sems = scratch
    columns = weights.shape[1]
    width = right_half.shape[1]
    start = lax.axis_index("dp") * columns
    copies = []
    for t in range(2):
        layer = 2 * group + t
        rows = slice(t * RANK, (t + 1) * RANK)
        right = right_half[rows, :]
        turned = jnp.dot(
            root[:, rows],
            pltpu.roll(right, lax.rem(width - start, width), 1)[:, :LR],
            precision=HIGH,
            preferred_element_type=jnp.float32,
        )
        change = lax.dot_general(
            turned,
            factor[rows, :],
            (((0,), (0,)), ((), ())),
            precision=HIGH,
            preferred_element_type=jnp.float32,
        )[:columns, :]
        square = jnp.sum(right * right) / (RANK * width)
        buf_b[t] = right * lax.rsqrt(jnp.full((1, 1), square, jnp.float32) + 1e-12)
        momentum_now = 0.8 * momentum[layer] + change
        buf_m[t] = momentum_now
        buf_w[t] = weights[layer] - 0.05 * momentum_now
        for k, (buf, out) in enumerate(((buf_b, new_b), (buf_m, new_m), (buf_w, new_w))):
            copies.append(pltpu.make_async_copy(buf.at[t], out.at[layer], sems.at[3 * t + k]))
            copies[-1].start()
    return copies


def last_mine_kernel(right_half, root, factor, weights, momentum, *refs):
    core = lax.rem(lax.axis_index("tp"), 2)
    root = unpacked(root)
    for copy in last_kernel(core, right_half, root, factor, weights, momentum, refs[:3], refs[3:]):
        copy.wait()


def last_other_kernel(replicas, right_half, left, weights, momentum, *refs):
    other = 1 - lax.rem(lax.axis_index("tp"), 2)
    factor = refs[-1]
    root = unpacked(right_half[HALF:, : 4 * HALF])
    solve_left(replicas, root, left, other, factor)
    for copy in last_kernel(other, right_half, root, factor, weights, momentum, refs[3:6], refs[6:-1]):
        copy.wait()


def last_half(kernel, right_half, operands, weights, momentum, outs=()):
    block = pl.BlockSpec(memory_space=pltpu.VMEM)
    anywhere = pl.BlockSpec(memory_space=pl.ANY)
    columns, rows = weights.shape[1:]
    width = right_half.shape[1]
    whole = jax.ShapeDtypeStruct(weights.shape, jnp.float32)
    basis = jax.ShapeDtypeStruct((LAYERS, RANK, width), jnp.float32)
    inputs = (right_half, *operands, weights, momentum)
    factor = [pltpu.VMEM((HALF, rows), jnp.float32)] * bool(outs)
    return pl.pallas_call(
        kernel,
        out_shape=[whole, basis, whole],
        in_specs=[block] * len(inputs) + [anywhere] * len(outs),
        out_specs=[anywhere] * 3,
        scratch_shapes=[
            pltpu.VMEM((2, columns, rows), jnp.float32),
            pltpu.VMEM((2, RANK, width), jnp.float32),
            pltpu.VMEM((2, columns, rows), jnp.float32),
            pltpu.SemaphoreType.DMA((6,)),
        ]
        + factor,
        input_output_aliases={len(inputs) + k: k for k in range(len(outs))},
        cost_estimate=pl.CostEstimate(flops=20_000_000, bytes_accessed=1_000_000, transcendentals=0),
        compiler_params=SMALL,
    )(*inputs, *outs)


def one_step(gradients, right_factor, weights_before, momentum):
    width = right_factor.shape[1]
    own, *others = left_parts(gradients, jnp.swapaxes(right_factor, 1, 2))
    one, two, three = to_ring(others, X_RINGS)
    share = sum_of_ring((own + two) + (one + three), Z_RINGS)
    pieces = [share] + to_ring([share] * 3, X_RINGS)

    send, keep_gram, keep_small, left = right_send(gradients, pieces)
    came = lax.ppermute(send, "tp", CORE_PAIRS)
    pair = right_keep(gradients, keep_small) + came[:HALF]
    gram = jnp.broadcast_to((keep_gram + came[HALF:, : 4 * HALF])[None], (8, 8, 4 * HALF))
    packet = jnp.concatenate([pair.reshape(8, 8, width), gram], axis=2)
    packet = lax.all_to_all(packet, "tp", 0, 0, tiled=True, axis_index_groups=CHIP_GROUPS)
    packet = jnp.sum(packet, axis=0)
    replicas = lax.axis_size("dp")
    root, factor = inverse_roots(replicas, packet[:, width:], left)
    share = sum_of_ring(packet[:, :width], X_RINGS)
    share = sum_of_ring(share, Z_RINGS)
    mine = lax.all_to_all(
        jnp.broadcast_to(share[None], (8, 8, width)), "tp", 0, 0, tiled=True, axis_index_groups=CHIP_GROUPS
    ).reshape(HALF, width)
    going = jnp.concatenate([mine, jnp.pad(root, ((0, 0), (0, width - 4 * HALF)))], axis=0)
    other = lax.ppermute(going, "tp", CORE_PAIRS)
    state = jnp.swapaxes(weights_before, 1, 2), jnp.swapaxes(momentum, 1, 2)
    outs = last_half(last_mine_kernel, mine, (root, factor), *state)
    outs = last_half(lambda *refs: last_other_kernel(replicas, *refs), other, (left,), *state, outs)
    return tuple(jnp.swapaxes(array, 1, 2) for array in outs)


def solution(mesh):
    return jax.shard_map(
        one_step,
        mesh=mesh,
        in_specs=(P("dp", None, "tp", None), P(), P(None, "tp", "dp"), P(None, "tp", "dp")),
        out_specs=(P(None, "tp", "dp"), P(), P(None, "tp", "dp")),
        check_vma=False,
    )
```

```python
import jax
import jax.numpy as jnp
from jax import lax
from jax.experimental import pallas as pl
from jax.experimental.pallas import tpu as pltpu
from jax.sharding import PartitionSpec as P


RANK = 32
LAYERS = 4
LR = LAYERS * RANK
HALF = LR // 2
HIGH = lax.Precision.HIGHEST
SMALL = pltpu.CompilerParams(vmem_limit_bytes=16 * 2**20)

X_RINGS = [[z * 4 + x for x in range(4)] for z in range(4)]
Z_RINGS = [[z * 4 + x for z in range(4)] for x in range(4)]
CORE_PAIRS = [(j, j ^ 1) for j in range(16)]
CHIP_GROUPS = [[2 * chip + core for chip in range(8)] for core in range(2)]


def hop(rings, step):
    return [(ring[j], ring[(j + step) % len(ring)]) for ring in rings for j in range(len(ring))]


def to_ring(arrays, rings):
    got = []
    for k, array in enumerate(arrays, 1):
        got.append(lax.ppermute(array, "dp", hop(rings, k)))
    return got


def sum_of_ring(array, rings):
    one, two, three = to_ring([array] * 3, rings)
    return (array + two) + (one + three)


def left_kernel(grads, basis, own, one, two, three, total_t, total):
    step = pl.program_id(0)
    layers = grads.shape[0]
    for l in range(layers):
        start = pl.multiple_of((step * layers + l) * RANK, RANK)
        total_t[pl.ds(start, RANK), :] = lax.dot_general(
            basis[l].astype(jnp.bfloat16), grads[l], (((1,), (1,)), ((), ())), preferred_element_type=jnp.float32
        )

    @pl.when(step == pl.num_programs(0) - 1)
    def _():
        total[...] = total_t[...].T
        rows = own.shape[0]
        x = lax.rem(lax.axis_index("dp"), 4)
        for back, out in enumerate((own, one, two, three)):
            start = lax.rem(x + back, 4) * rows
            out[...] = total[pl.ds(pl.multiple_of(start, 8), rows), :]


def left_parts(grads, basis_t):
    _, layers, rows, width = grads.shape
    piece = jax.ShapeDtypeStruct((rows // 4, LR), jnp.float32)
    return pl.pallas_call(
        left_kernel,
        out_shape=[piece] * 4,
        grid=(2,),
        in_specs=[
            pl.BlockSpec((None, layers // 2, rows, width), lambda l: (0, l, 0, 0)),
            pl.BlockSpec((layers // 2, RANK, width), lambda l: (l, 0, 0)),
        ],
        out_specs=[pl.BlockSpec((rows // 4, LR), lambda l: (0, 0))] * 4,
        scratch_shapes=[pltpu.VMEM((LR, rows), jnp.float32), pltpu.VMEM((rows, LR), jnp.float32)],
        compiler_params=pltpu.CompilerParams(vmem_limit_bytes=54772 * 2**10),
        name="left_parts",
    )(grads, basis_t)


def right_send_kernel(grads, own, one, two, three, send, keep_gram, keep_small, left):
    rows = own.shape[0]
    x = lax.rem(lax.axis_index("dp"), 4)
    core = lax.rem(lax.axis_index("tp"), 2)
    for back, piece in enumerate((own, one, two, three)):
        start = lax.rem(x + 4 - back, 4) * rows
        left[pl.ds(pl.multiple_of(start, 8), rows), :] = piece[...]
    whole = left[...]
    small = whole.T.astype(jnp.bfloat16)
    low, high = small[:HALF, :], small[HALF:, :]
    keep_small[...] = jnp.where(core == 0, low, high)
    going = jnp.where(core == 0, high, low)
    for t in range(2):
        send[t * RANK : (t + 1) * RANK, :] = jnp.dot(
            going[t * RANK : (t + 1) * RANK, :],
            grads[0, 2 * (1 - core) + t],
            preferred_element_type=jnp.float32,
        )
    full = lax.dot_general(
        whole, whole, (((0,), (0,)), ((), ())), precision=HIGH, preferred_element_type=jnp.float32
    )
    blocks = [full[l * RANK : (l + 1) * RANK, l * RANK : (l + 1) * RANK] for l in range(LAYERS)]
    first, second = (jnp.concatenate(blocks[h : h + 2], axis=1) for h in (0, 2))
    kept = jnp.where(core == 0, first, second)
    gone = jnp.where(core == 0, second, first)
    for k in range(4):
        lanes = slice(k * HALF, (k + 1) * HALF)
        keep_gram[:, lanes] = kept[8 * k : 8 * k + 8, :]
        send[HALF : HALF + 8, lanes] = gone[8 * k : 8 * k + 8, :]
    send[HALF : HALF + 8, 4 * HALF :] = jnp.zeros((8, send.shape[1] - 4 * HALF), jnp.float32)


def right_send(grads, pieces):
    _, _, rows, width = grads.shape
    block = pl.BlockSpec(memory_space=pltpu.VMEM)
    return pl.pallas_call(
        right_send_kernel,
        out_shape=[
            jax.ShapeDtypeStruct((HALF + 8, width), jnp.float32),
            jax.ShapeDtypeStruct((8, 4 * HALF), jnp.float32),
            jax.ShapeDtypeStruct((HALF, rows), jnp.bfloat16),
            jax.ShapeDtypeStruct((rows, LR), jnp.float32),
        ],
        in_specs=[block] * 5,
        out_specs=[block] * 4,
        compiler_params=SMALL,
        name="right_send",
    )(grads, *pieces)


def right_keep_kernel(grads, small, keep):
    core = lax.rem(lax.axis_index("tp"), 2)
    for t in range(2):
        keep[t * RANK : (t + 1) * RANK, :] = jnp.dot(
            small[t * RANK : (t + 1) * RANK, :], grads[0, 2 * core + t], preferred_element_type=jnp.float32
        )


def right_keep(grads, small):
    block = pl.BlockSpec(memory_space=pltpu.VMEM)
    return pl.pallas_call(
        right_keep_kernel,
        out_shape=jax.ShapeDtypeStruct((HALF, grads.shape[3]), jnp.float32),
        in_specs=[block] * 2,
        out_specs=block,
        cost_estimate=pl.CostEstimate(flops=52_000_000, bytes_accessed=2_000_000, transcendentals=0),
        compiler_params=SMALL,
        name="right_keep",
    )(grads, small)


def unpacked(packed):
    return jnp.concatenate([packed[:, k * HALF : (k + 1) * HALF] for k in range(4)], axis=0)


def solve_left(replicas, root, left, group, out):
    factor = jnp.where(group == 0, left[:, :HALF], left[:, HALF:])
    for t in range(2):
        lanes = slice(t * RANK, (t + 1) * RANK)
        out[lanes, :] = (
            lax.dot_general(
                root[:, lanes],
                factor[:, lanes],
                (((1,), (1,)), ((), ())),
                precision=HIGH,
                preferred_element_type=jnp.float32,
            )
            / replicas
        )


def root_kernel(replicas, packed, left, out, factor):
    gram = unpacked(packed)
    row = lax.broadcasted_iota(jnp.int32, (RANK, LR), 0)
    lane = lax.broadcasted_iota(jnp.int32, (RANK, LR), 1)
    first = (lane // RANK) % 2 == 0
    one = jnp.where(lane % RANK == row, 1.0, 0.0)
    ridge = jnp.zeros((RANK, HALF), jnp.float32)
    for l in range(2):
        mine = lane[:, :HALF] // RANK == l
        on_diagonal = mine & (lane[:, :HALF] % RANK == row[:, :HALF])
        mean = jnp.sum(jnp.where(on_diagonal, gram, 0.0)) / RANK
        ridge = jnp.where(on_diagonal, 0.001 * mean, ridge)
    m = jnp.concatenate([gram + ridge, one[:, HALF:]], axis=1)
    for k in range(RANK - 1):
        column = jnp.where(first, m[:, k : k + 1], m[:, RANK + k : RANK + k + 1])
        scale = jnp.where(row > k, column * (1.0 / column[k : k + 1, :]), 0.0)
        m = m - scale * m[k : k + 1, :]
    pivots = [
        jnp.sum(jnp.where(lane == row + l * RANK, m, 0.0), axis=1, keepdims=True) for l in range(2)
    ]
    pivot = jnp.where(first, pivots[0], pivots[1])[:, HALF:]
    shrink = lax.rsqrt(pivot)
    shrink = shrink * (1.5 - 0.5 * (pivot * shrink) * shrink)
    root = m[:, HALF:] * shrink
    for k in range(4):
        out[:, k * HALF : (k + 1) * HALF] = root[8 * k : 8 * k + 8, :]
    solve_left(replicas, root, left, lax.rem(lax.axis_index("tp"), 2), factor)


def inverse_roots(replicas, packed, left):
    return pl.pallas_call(
        lambda *refs: root_kernel(replicas, *refs),
        out_shape=[
            jax.ShapeDtypeStruct((8, 4 * HALF), jnp.float32),
            jax.ShapeDtypeStruct((HALF, left.shape[0]), jnp.float32),
        ],
        in_specs=[pl.BlockSpec(memory_space=pltpu.VMEM)] * 2,
        out_specs=[pl.BlockSpec(memory_space=pltpu.VMEM)] * 2,
        cost_estimate=pl.CostEstimate(flops=20_000_000, bytes_accessed=32768, transcendentals=0),
        compiler_params=SMALL,
        name="inverse_roots",
    )(packed, left)


def start_copy(copies, buf, out, layer, t, sem):
    copies.append(pltpu.make_async_copy(buf.at[t], out.at[layer], sem))
    copies[-1].start()


def basis_part(group, right_half, new_b, buf_b, sems):
    copies = []
    width = right_half.shape[1]
    for t in range(2):
        right = right_half[t * RANK : (t + 1) * RANK, :]
        square = jnp.sum(right * right) / (RANK * width)
        buf_b[t] = right * lax.rsqrt(jnp.full((1, 1), square, jnp.float32) + 1e-12)
        start_copy(copies, buf_b, new_b, 2 * group + t, t, sems.at[t])
    return copies


def reduced_right(right_half, root, columns):
    width = right_half.shape[1]
    start = lax.axis_index("dp") * columns
    turned = pltpu.roll(right_half[:HALF, :], lax.rem(width - start, width), 1)[:, :LR]
    return [
        jnp.dot(
            root[:, t * RANK : (t + 1) * RANK],
            turned[t * RANK : (t + 1) * RANK, :],
            precision=HIGH,
            preferred_element_type=jnp.float32,
        )
        for t in range(2)
    ]


def state_part(group, reduced, factor, weights, momentum, new_w, new_m, buf_w, buf_m, sems):
    copies = []
    columns = weights.shape[1]
    changes = [
        lax.dot_general(
            reduced[t][:, :columns],
            factor[t * RANK : (t + 1) * RANK, :],
            (((0,), (0,)), ((), ())),
            precision=HIGH,
            preferred_element_type=jnp.float32,
        )
        for t in range(2)
    ]
    for t, change in enumerate(changes):
        layer = 2 * group + t
        momentum_now = 0.8 * momentum[layer] + change
        buf_m[t] = momentum_now
        start_copy(copies, buf_m, new_m, layer, t, sems.at[2 + t])
        buf_w[t] = weights[layer] - 0.05 * momentum_now
        start_copy(copies, buf_w, new_w, layer, t, sems.at[4 + t])
    return copies


def last_mine_kernel(
    right_half, root, factor, weights, momentum, new_w, new_b, new_m, buf_w, buf_b, buf_m, sems
):
    core = lax.rem(lax.axis_index("tp"), 2)
    reduced = reduced_right(right_half, unpacked(root), weights.shape[1])
    copies = basis_part(core, right_half, new_b, buf_b, sems)
    copies += state_part(core, reduced, factor, weights, momentum, new_w, new_m, buf_w, buf_m, sems)
    for copy in copies:
        copy.wait()


def last_other_kernel(replicas, right_half, left, weights, momentum, *refs):
    new_w, new_b, new_m, buf_w, buf_b, buf_m, sems, factor = refs[3:]
    other = 1 - lax.rem(lax.axis_index("tp"), 2)
    root = unpacked(right_half[HALF:, : 4 * HALF])
    reduced = reduced_right(right_half, root, weights.shape[1])
    solve_left(replicas, root, left, other, factor)
    copies = basis_part(other, right_half, new_b, buf_b, sems)
    copies += state_part(other, reduced, factor, weights, momentum, new_w, new_m, buf_w, buf_m, sems)
    for copy in copies:
        copy.wait()


def last_half(kernel, right_half, operands, weights, momentum, outs=()):
    block = pl.BlockSpec(memory_space=pltpu.VMEM)
    anywhere = pl.BlockSpec(memory_space=pl.ANY)
    columns, rows = weights.shape[1:]
    width = right_half.shape[1]
    whole = jax.ShapeDtypeStruct(weights.shape, jnp.float32)
    basis = jax.ShapeDtypeStruct((LAYERS, RANK, width), jnp.float32)
    inputs = (right_half, *operands, weights, momentum)
    factor = [pltpu.VMEM((HALF, rows), jnp.float32)] * bool(outs)
    return pl.pallas_call(
        kernel,
        out_shape=[whole, basis, whole],
        in_specs=[block] * len(inputs) + [anywhere] * len(outs),
        out_specs=[anywhere] * 3,
        scratch_shapes=[
            pltpu.VMEM((2, columns, rows), jnp.float32),
            pltpu.VMEM((2, RANK, width), jnp.float32),
            pltpu.VMEM((2, columns, rows), jnp.float32),
            pltpu.SemaphoreType.DMA((6,)),
        ]
        + factor,
        input_output_aliases={len(inputs) + k: k for k in range(len(outs))},
        cost_estimate=pl.CostEstimate(flops=20_000_000, bytes_accessed=1_000_000, transcendentals=0),
        compiler_params=SMALL,
    )(*inputs, *outs)


def one_step(gradients, right_factor, weights_before, momentum):
    width = right_factor.shape[1]
    own, *others = left_parts(gradients, jnp.swapaxes(right_factor, 1, 2))
    one, two, three = to_ring(others, X_RINGS)
    share = sum_of_ring((own + two) + (one + three), Z_RINGS)
    pieces = [share] + to_ring([share] * 3, X_RINGS)

    send, keep_gram, keep_small, left = right_send(gradients, pieces)
    came = lax.ppermute(send, "tp", CORE_PAIRS)
    pair = right_keep(gradients, keep_small) + came[:HALF]
    gram = jnp.broadcast_to((keep_gram + came[HALF:, : 4 * HALF])[None], (8, 8, 4 * HALF))
    packet = jnp.concatenate([pair.reshape(8, 8, width), gram], axis=2)
    packet = lax.all_to_all(packet, "tp", 0, 0, tiled=True, axis_index_groups=CHIP_GROUPS)
    packet = jnp.sum(packet, axis=0)
    replicas = lax.axis_size("dp")
    root, factor = inverse_roots(replicas, packet[:, width:], left)
    share = sum_of_ring(packet[:, :width], X_RINGS)
    share = sum_of_ring(share, Z_RINGS)
    mine = lax.all_to_all(
        jnp.broadcast_to(share[None], (8, 8, width)), "tp", 0, 0, tiled=True, axis_index_groups=CHIP_GROUPS
    ).reshape(HALF, width)
    going = jnp.concatenate([mine, jnp.pad(root, ((0, 0), (0, width - 4 * HALF)))], axis=0)
    other = lax.ppermute(going, "tp", CORE_PAIRS)
    state = jnp.swapaxes(weights_before, 1, 2), jnp.swapaxes(momentum, 1, 2)
    outs = last_half(last_mine_kernel, mine, (root, factor), *state)
    outs = last_half(lambda *refs: last_other_kernel(replicas, *refs), other, (left,), *state, outs)
    return tuple(jnp.swapaxes(array, 1, 2) for array in outs)


def solution(mesh):
    return jax.shard_map(
        one_step,
        mesh=mesh,
        in_specs=(P("dp", None, "tp", None), P(), P(None, "tp", "dp"), P(None, "tp", "dp")),
        out_specs=(P(None, "tp", "dp"), P(), P(None, "tp", "dp")),
        check_vma=False,
    )
```

```python
import jax
import jax.numpy as jnp
from jax import lax
from jax.experimental import pallas as pl
from jax.experimental.pallas import tpu as pltpu
from jax.sharding import PartitionSpec as P


RANK = 32
LAYERS = 4
LR = LAYERS * RANK
HALF = LR // 2
HIGH = lax.Precision.HIGHEST
SMALL = pltpu.CompilerParams(vmem_limit_bytes=16 * 2**20)

X_RINGS = [[z * 4 + x for x in range(4)] for z in range(4)]
Z_RINGS = [[z * 4 + x for z in range(4)] for x in range(4)]
CORE_PAIRS = [(j, j ^ 1) for j in range(16)]
CHIP_GROUPS = [[2 * chip + core for chip in range(8)] for core in range(2)]


def hop(rings, step):
    return [(ring[j], ring[(j + step) % len(ring)]) for ring in rings for j in range(len(ring))]


def to_ring(arrays, rings):
    got = []
    for k, array in enumerate(arrays, 1):
        got.append(lax.ppermute(array, "dp", hop(rings, k)))
    return got


def sum_of_ring(array, rings):
    one, two, three = to_ring([array] * 3, rings)
    return (array + two) + (one + three)


def left_kernel(grads, basis, own, one, two, three, total_t, total):
    step = pl.program_id(0)
    layers = grads.shape[0]
    for l in range(layers):
        start = pl.multiple_of((step * layers + l) * RANK, RANK)
        total_t[pl.ds(start, RANK), :] = lax.dot_general(
            basis[l].astype(jnp.bfloat16), grads[l], (((1,), (1,)), ((), ())), preferred_element_type=jnp.float32
        )

    @pl.when(step == pl.num_programs(0) - 1)
    def _():
        total[...] = total_t[...].T
        rows = own.shape[0]
        x = lax.rem(lax.axis_index("dp"), 4)
        for back, out in enumerate((own, one, two, three)):
            start = lax.rem(x + back, 4) * rows
            out[...] = total[pl.ds(pl.multiple_of(start, 8), rows), :]


def left_parts(grads, basis_t):
    _, layers, rows, width = grads.shape
    piece = jax.ShapeDtypeStruct((rows // 4, LR), jnp.float32)
    return pl.pallas_call(
        left_kernel,
        out_shape=[piece] * 4,
        grid=(2,),
        in_specs=[
            pl.BlockSpec((None, layers // 2, rows, width), lambda l: (0, l, 0, 0)),
            pl.BlockSpec((layers // 2, RANK, width), lambda l: (l, 0, 0)),
        ],
        out_specs=[pl.BlockSpec((rows // 4, LR), lambda l: (0, 0))] * 4,
        scratch_shapes=[pltpu.VMEM((LR, rows), jnp.float32), pltpu.VMEM((rows, LR), jnp.float32)],
        compiler_params=pltpu.CompilerParams(vmem_limit_bytes=54772 * 2**10),
        name="left_parts",
    )(grads, basis_t)


def right_send_kernel(grads, own, one, two, three, send, keep_gram, keep_small, left):
    rows = own.shape[0]
    x = lax.rem(lax.axis_index("dp"), 4)
    core = lax.rem(lax.axis_index("tp"), 2)
    for back, piece in enumerate((own, one, two, three)):
        start = lax.rem(x + 4 - back, 4) * rows
        left[pl.ds(pl.multiple_of(start, 8), rows), :] = piece[...]
    whole = left[...]
    small = whole.T.astype(jnp.bfloat16)
    low, high = small[:HALF, :], small[HALF:, :]
    keep_small[...] = jnp.where(core == 0, low, high)
    going = jnp.where(core == 0, high, low)
    for t in range(2):
        send[t * RANK : (t + 1) * RANK, :] = jnp.dot(
            going[t * RANK : (t + 1) * RANK, :],
            grads[0, 2 * (1 - core) + t],
            preferred_element_type=jnp.float32,
        )
    full = lax.dot_general(
        whole, whole, (((0,), (0,)), ((), ())), precision=HIGH, preferred_element_type=jnp.float32
    )
    blocks = [full[l * RANK : (l + 1) * RANK, l * RANK : (l + 1) * RANK] for l in range(LAYERS)]
    first, second = (jnp.concatenate(blocks[h : h + 2], axis=1) for h in (0, 2))
    kept = jnp.where(core == 0, first, second)
    gone = jnp.where(core == 0, second, first)
    for k in range(4):
        lanes = slice(k * HALF, (k + 1) * HALF)
        keep_gram[:, lanes] = kept[8 * k : 8 * k + 8, :]
        send[HALF : HALF + 8, lanes] = gone[8 * k : 8 * k + 8, :]
    send[HALF : HALF + 8, 4 * HALF :] = jnp.zeros((8, send.shape[1] - 4 * HALF), jnp.float32)


def right_send(grads, pieces):
    _, _, rows, width = grads.shape
    block = pl.BlockSpec(memory_space=pltpu.VMEM)
    return pl.pallas_call(
        right_send_kernel,
        out_shape=[
            jax.ShapeDtypeStruct((HALF + 8, width), jnp.float32),
            jax.ShapeDtypeStruct((8, 4 * HALF), jnp.float32),
            jax.ShapeDtypeStruct((HALF, rows), jnp.bfloat16),
            jax.ShapeDtypeStruct((rows, LR), jnp.float32),
        ],
        in_specs=[block] * 5,
        out_specs=[block] * 4,
        compiler_params=SMALL,
        name="right_send",
    )(grads, *pieces)


def right_keep_kernel(grads, small, keep):
    core = lax.rem(lax.axis_index("tp"), 2)
    for t in range(2):
        keep[t * RANK : (t + 1) * RANK, :] = jnp.dot(
            small[t * RANK : (t + 1) * RANK, :], grads[0, 2 * core + t], preferred_element_type=jnp.float32
        )


def right_keep(grads, small):
    block = pl.BlockSpec(memory_space=pltpu.VMEM)
    return pl.pallas_call(
        right_keep_kernel,
        out_shape=jax.ShapeDtypeStruct((HALF, grads.shape[3]), jnp.float32),
        in_specs=[block] * 2,
        out_specs=block,
        cost_estimate=pl.CostEstimate(flops=52_000_000, bytes_accessed=2_000_000, transcendentals=0),
        compiler_params=SMALL,
        name="right_keep",
    )(grads, small)


def unpacked(packed):
    return jnp.concatenate([packed[:, k * HALF : (k + 1) * HALF] for k in range(4)], axis=0)


def solve_left(replicas, root, left, group, out):
    factor = jnp.where(group == 0, left[:, :HALF], left[:, HALF:])
    for t in range(2):
        lanes = slice(t * RANK, (t + 1) * RANK)
        out[lanes, :] = (
            lax.dot_general(
                root[:, lanes],
                factor[:, lanes],
                (((1,), (1,)), ((), ())),
                precision=HIGH,
                preferred_element_type=jnp.float32,
            )
            / replicas
        )


def root_kernel(replicas, packed, left, out, factor):
    gram = unpacked(packed)
    row = lax.broadcasted_iota(jnp.int32, (RANK, LR), 0)
    lane = lax.broadcasted_iota(jnp.int32, (RANK, LR), 1)
    first = (lane // RANK) % 2 == 0
    one = jnp.where(lane % RANK == row, 1.0, 0.0)
    ridge = jnp.zeros((RANK, HALF), jnp.float32)
    for l in range(2):
        mine = lane[:, :HALF] // RANK == l
        on_diagonal = mine & (lane[:, :HALF] % RANK == row[:, :HALF])
        mean = jnp.sum(jnp.where(on_diagonal, gram, 0.0)) / RANK
        ridge = jnp.where(on_diagonal, 0.001 * mean, ridge)
    m = jnp.concatenate([gram + ridge, one[:, HALF:]], axis=1)
    for k in range(RANK - 1):
        column = jnp.where(first, m[:, k : k + 1], m[:, RANK + k : RANK + k + 1])
        scale = jnp.where(row > k, column * (1.0 / column[k : k + 1, :]), 0.0)
        m = m - scale * m[k : k + 1, :]
    pivots = [
        jnp.sum(jnp.where(lane == row + l * RANK, m, 0.0), axis=1, keepdims=True) for l in range(2)
    ]
    pivot = jnp.where(first, pivots[0], pivots[1])[:, HALF:]
    shrink = lax.rsqrt(pivot)
    shrink = shrink * (1.5 - 0.5 * (pivot * shrink) * shrink)
    root = m[:, HALF:] * shrink
    for k in range(4):
        out[:, k * HALF : (k + 1) * HALF] = root[8 * k : 8 * k + 8, :]
    solve_left(replicas, root, left, lax.rem(lax.axis_index("tp"), 2), factor)


def inverse_roots(replicas, packed, left):
    return pl.pallas_call(
        lambda *refs: root_kernel(replicas, *refs),
        out_shape=[
            jax.ShapeDtypeStruct((8, 4 * HALF), jnp.float32),
            jax.ShapeDtypeStruct((HALF, left.shape[0]), jnp.float32),
        ],
        in_specs=[pl.BlockSpec(memory_space=pltpu.VMEM)] * 2,
        out_specs=[pl.BlockSpec(memory_space=pltpu.VMEM)] * 2,
        cost_estimate=pl.CostEstimate(flops=20_000_000, bytes_accessed=32768, transcendentals=0),
        compiler_params=SMALL,
        name="inverse_roots",
    )(packed, left)


def start_copy(copies, buf, out, layer, t, sem):
    copies.append(pltpu.make_async_copy(buf.at[t], out.at[layer], sem))
    copies[-1].start()


def basis_part(group, right_half, new_b, buf_b, sems):
    copies = []
    width = right_half.shape[1]
    for t in range(2):
        right = right_half[t * RANK : (t + 1) * RANK, :]
        square = jnp.sum(right * right) / (RANK * width)
        buf_b[t] = right * lax.rsqrt(jnp.full((1, 1), square, jnp.float32) + 1e-12)
        start_copy(copies, buf_b, new_b, 2 * group + t, t, sems.at[t])
    return copies


def reduced_right(right_half, root, columns):
    width = right_half.shape[1]
    start = lax.axis_index("dp") * columns
    turned = pltpu.roll(right_half[:HALF, :], lax.rem(width - start, width), 1)[:, :LR]
    return [
        jnp.dot(
            root[:, t * RANK : (t + 1) * RANK],
            turned[t * RANK : (t + 1) * RANK, :],
            precision=HIGH,
            preferred_element_type=jnp.float32,
        )
        for t in range(2)
    ]


def halves(array):
    high = array.astype(jnp.bfloat16)
    return high, (array - high.astype(jnp.float32)).astype(jnp.bfloat16)


def state_part(group, reduced, factor, weights, momentum, new_w, new_m, buf_w, buf_m, sems):
    copies = []
    columns = weights.shape[1]
    changes = []
    for t in range(2):
        right_high, right_low = halves(reduced[t][:, :columns])
        left_high, left_low = halves(factor[t * RANK : (t + 1) * RANK, :])
        changes.append(
            lax.dot_general(
                jnp.concatenate([right_high, right_high, right_low], axis=0),
                jnp.concatenate([left_high, left_low, left_high], axis=0),
                (((0,), (0,)), ((), ())),
                preferred_element_type=jnp.float32,
            )
        )
    for t, change in enumerate(changes):
        layer = 2 * group + t
        momentum_now = 0.8 * momentum[layer] + change
        buf_m[t] = momentum_now
        start_copy(copies, buf_m, new_m, layer, t, sems.at[2 + t])
        buf_w[t] = weights[layer] - 0.05 * momentum_now
        start_copy(copies, buf_w, new_w, layer, t, sems.at[4 + t])
    return copies


def last_mine_kernel(
    right_half, root, factor, weights, momentum, new_w, new_b, new_m, buf_w, buf_b, buf_m, sems
):
    core = lax.rem(lax.axis_index("tp"), 2)
    reduced = reduced_right(right_half, unpacked(root), weights.shape[1])
    copies = basis_part(core, right_half, new_b, buf_b, sems)
    copies += state_part(core, reduced, factor, weights, momentum, new_w, new_m, buf_w, buf_m, sems)
    for copy in copies:
        copy.wait()


def last_other_kernel(replicas, right_half, left, weights, momentum, *refs):
    new_w, new_b, new_m, buf_w, buf_b, buf_m, sems, factor = refs[3:]
    other = 1 - lax.rem(lax.axis_index("tp"), 2)
    root = unpacked(right_half[HALF:, : 4 * HALF])
    reduced = reduced_right(right_half, root, weights.shape[1])
    solve_left(replicas, root, left, other, factor)
    copies = basis_part(other, right_half, new_b, buf_b, sems)
    copies += state_part(other, reduced, factor, weights, momentum, new_w, new_m, buf_w, buf_m, sems)
    for copy in copies:
        copy.wait()


def last_half(kernel, right_half, operands, weights, momentum, outs=()):
    block = pl.BlockSpec(memory_space=pltpu.VMEM)
    anywhere = pl.BlockSpec(memory_space=pl.ANY)
    columns, rows = weights.shape[1:]
    width = right_half.shape[1]
    whole = jax.ShapeDtypeStruct(weights.shape, jnp.float32)
    basis = jax.ShapeDtypeStruct((LAYERS, RANK, width), jnp.float32)
    inputs = (right_half, *operands, weights, momentum)
    factor = [pltpu.VMEM((HALF, rows), jnp.float32)] * bool(outs)
    return pl.pallas_call(
        kernel,
        out_shape=[whole, basis, whole],
        in_specs=[block] * len(inputs) + [anywhere] * len(outs),
        out_specs=[anywhere] * 3,
        scratch_shapes=[
            pltpu.VMEM((2, columns, rows), jnp.float32),
            pltpu.VMEM((2, RANK, width), jnp.float32),
            pltpu.VMEM((2, columns, rows), jnp.float32),
            pltpu.SemaphoreType.DMA((6,)),
        ]
        + factor,
        input_output_aliases={len(inputs) + k: k for k in range(len(outs))},
        cost_estimate=pl.CostEstimate(flops=20_000_000, bytes_accessed=1_000_000, transcendentals=0),
        compiler_params=SMALL,
    )(*inputs, *outs)


def one_step(gradients, right_factor, weights_before, momentum):
    width = right_factor.shape[1]
    own, *others = left_parts(gradients, jnp.swapaxes(right_factor, 1, 2))
    one, two, three = to_ring(others, X_RINGS)
    share = sum_of_ring((own + two) + (one + three), Z_RINGS)
    pieces = [share] + to_ring([share] * 3, X_RINGS)

    send, keep_gram, keep_small, left = right_send(gradients, pieces)
    came = lax.ppermute(send, "tp", CORE_PAIRS)
    pair = right_keep(gradients, keep_small) + came[:HALF]
    gram = jnp.broadcast_to((keep_gram + came[HALF:, : 4 * HALF])[None], (8, 8, 4 * HALF))
    packet = jnp.concatenate([pair.reshape(8, 8, width), gram], axis=2)
    packet = lax.all_to_all(packet, "tp", 0, 0, tiled=True, axis_index_groups=CHIP_GROUPS)
    packet = jnp.sum(packet, axis=0)
    replicas = lax.axis_size("dp")
    root, factor = inverse_roots(replicas, packet[:, width:], left)
    share = sum_of_ring(packet[:, :width], X_RINGS)
    share = sum_of_ring(share, Z_RINGS)
    mine = lax.all_to_all(
        jnp.broadcast_to(share[None], (8, 8, width)), "tp", 0, 0, tiled=True, axis_index_groups=CHIP_GROUPS
    ).reshape(HALF, width)
    going = jnp.concatenate([mine, jnp.pad(root, ((0, 0), (0, width - 4 * HALF)))], axis=0)
    other = lax.ppermute(going, "tp", CORE_PAIRS)
    state = jnp.swapaxes(weights_before, 1, 2), jnp.swapaxes(momentum, 1, 2)
    outs = last_half(last_mine_kernel, mine, (root, factor), *state)
    outs = last_half(lambda *refs: last_other_kernel(replicas, *refs), other, (left,), *state, outs)
    return tuple(jnp.swapaxes(array, 1, 2) for array in outs)


def solution(mesh):
    return jax.shard_map(
        one_step,
        mesh=mesh,
        in_specs=(P("dp", None, "tp", None), P(), P(None, "tp", "dp"), P(None, "tp", "dp")),
        out_specs=(P(None, "tp", "dp"), P(), P(None, "tp", "dp")),
        check_vma=False,
    )
```
